32 devices in a mesh: wide: 8 (over y, x, core), narrow: 4 (over z).
Axes of the slice: x: 2, y: 2, z: 4, core: 2. Of those that a mesh axis runs over, the one named last changes fastest.
Arguments:
- local_slopes: float32 [32, 512, 128], P(('wide', 'narrow')), may hold values from -0.25 to 0.25
- global_slopes: float32 [32, 512, 1024], P(('wide', 'narrow')), may hold values from -0.25 to 0.25
- residuals: float32 [32, 512], P(('wide', 'narrow')), may hold values from -6 to 6
- weights: float32 [32, 512], P(('wide', 'narrow')), may hold values from 0.1 to 10
- track_slot_count: int32 [32], P(('wide', 'narrow')), may hold values from 64 to 512
- windows: int32 [32], P(('wide', 'narrow')), may hold values from 0 to 3
Outputs:
- normal_matrix: float32 [4, 1024, 1024], P(None, 'narrow', 'wide')
- normal_rhs: float32 [4, 1024], P(None, 'narrow')
The draws below stay inside these ranges and needn't reach their ends.
All inputs are finite; a program needn't handle non-finite values.
Results may differ from the reference program's by a relative error of at most 0.0003.
Values sent between devices are 32-bit elements; how exact they have to be, the bound alone decides.
A program may use at most 64 MiB of HBM per device.

```python
import math
import jax
import jax.numpy as jnp
from jax import lax

WINDOW_PARAMS = 1024
LOCAL_PARAMS = 128
MEASURE_SLOTS = 512
NWIN = 4
TRACK_BUNDLES = 32


def set_ends(drawn, own_key, low, top_value):
    index_at = [jax.random.randint(jax.random.fold_in(own_key, axis), (), 0, length) for axis, length in enumerate(drawn.shape)]
    main_axis = drawn.shape.index(max(drawn.shape))
    next_to = index_at[:main_axis] + [(index_at[main_axis] + 1) % drawn.shape[main_axis]] + index_at[main_axis + 1:]
    return drawn.at[tuple(index_at)].set(low).at[tuple(next_to)].set(top_value)


def levels(stream_key, extent, shards, least, top_value):
    level = 1.0
    for dim, shards_of in shards:
        draws = jax.random.uniform(jax.random.fold_in(jax.random.fold_in(stream_key, 6), dim), (shards_of,), jnp.float32, least / len(shards), top_value / len(shards))
        level = level * jnp.repeat(jnp.exp(draws), extent[dim] // shards_of).reshape((-1,) + (1,) * (len(extent) - 1 - dim))
    return level


def bell_draw(key, dims, scale, most, shards=(), held_as=jnp.bfloat16):
    entries = scale * jax.random.normal(key, dims, jnp.float32)
    if shards:
        entries = entries * levels(key, dims, shards, -0.22, 0.18)
    return jnp.clip(entries, -most, most).astype(held_as)


def setup_inputs(seed: int = 0) -> dict:
    arg_keys = jax.random.split(jax.random.key(seed), 7)
    local_slopes = bell_draw(arg_keys[0], (TRACK_BUNDLES, MEASURE_SLOTS, LOCAL_PARAMS), MEASURE_SLOTS ** -0.5, 0.25, ((0, 32),), jnp.float32)
    global_slopes = bell_draw(arg_keys[1], (TRACK_BUNDLES, MEASURE_SLOTS, WINDOW_PARAMS), MEASURE_SLOTS ** -0.5, 0.25, ((0, 32),), jnp.float32)
    residuals = bell_draw(arg_keys[2], (TRACK_BUNDLES, MEASURE_SLOTS), 1.0, 6.0, ((0, 32),), jnp.float32)
    weights = jnp.clip(jnp.exp(math.log(10.0) - 4.6051702 * jax.random.uniform(arg_keys[3], (TRACK_BUNDLES, MEASURE_SLOTS), jnp.float32) ** levels(arg_keys[3], (TRACK_BUNDLES, MEASURE_SLOTS), ((0, 32),), -0.2, 0.2)), 0.1, 10.0)
    track_slot_count = set_ends(jax.random.randint(arg_keys[4], (TRACK_BUNDLES,), MEASURE_SLOTS // 8, MEASURE_SLOTS + 1), jax.random.fold_in(arg_keys[4], 1), MEASURE_SLOTS // 8, MEASURE_SLOTS).astype(jnp.int32)
    windows = set_ends(jax.random.randint(arg_keys[5], (TRACK_BUNDLES,), 0, NWIN), jax.random.fold_in(arg_keys[5], 1), 0, NWIN - 1).astype(jnp.int32)
    return {"local_slopes": local_slopes, "global_slopes": global_slopes, "residuals": residuals, "weights": weights, "track_slot_count": track_slot_count, "windows": windows}


def tdot(left, right):
    return lax.dot_general(left.astype(jnp.float32), right.astype(jnp.float32), (((0,), (0,)), ((), ())), precision=lax.Precision.HIGHEST, preferred_element_type=jnp.float32)

def reference(local_slopes, global_slopes, residuals, weights, track_slot_count, windows):
    slot_entries = jnp.arange(MEASURE_SLOTS, dtype=jnp.int32)

    def one_bundle(carry, items):
        matrix, rhs = carry
        local_b, global_b, resid_b, weight_b, count_b, window_b = items
        live = jnp.where(slot_entries < count_b, weight_b, jnp.float32(0.0))
        wl = local_b * live[:, None]
        wg = global_b * live[:, None]
        curv = tdot(wl, local_b) + jnp.eye(LOCAL_PARAMS, dtype=jnp.float32)
        coupling = tdot(wl, global_b)
        lr = tdot(wl, resid_b[:, None])
        gram = tdot(wg, global_b)
        gr = tdot(wg, resid_b[:, None])[:, 0]
        factor = jnp.linalg.cholesky(curv)
        solved = jax.scipy.linalg.cho_solve((factor, True), jnp.concatenate([coupling, lr], axis=1))
        schur = gram - tdot(coupling, solved[:, :WINDOW_PARAMS])
        srhs = gr - tdot(coupling, solved[:, WINDOW_PARAMS:])[:, 0]
        picks = (jnp.arange(NWIN, dtype=jnp.int32) == window_b).astype(jnp.float32)
        matrix = matrix + picks[:, None, None] * schur[None]
        rhs = rhs + picks[:, None] * srhs[None]
        return ((matrix, rhs), None)
    start = (jnp.zeros((NWIN, WINDOW_PARAMS, WINDOW_PARAMS), jnp.float32), jnp.zeros((NWIN, WINDOW_PARAMS), jnp.float32))
    (matrix, rhs), _ = lax.scan(one_bundle, start, (local_slopes, global_slopes, residuals, weights, track_slot_count, windows))
    return (matrix, rhs)
```

```python
import functools
import jax
import jax.numpy as jnp
from jax import lax
from jax.experimental import pallas as pl
from jax.experimental.pallas import tpu as pltpu
from jax.sharding import PartitionSpec as P

WINDOW_PARAMS = 1024
NWIN = 4
LANES = 128
SUB = 8
PANEL = 64
CUT = 64
AHEAD = 2
LAG = 1
MESH = pl.DeviceIdType.MESH
HIGHEST = lax.Precision.HIGHEST
HIGH = lax.Precision.HIGH


def tdot(left, right, precision=HIGHEST):
    return lax.dot_general(
        left,
        right,
        (((0,), (0,)), ((), ())),
        precision=precision,
        preferred_element_type=jnp.float32,
    )


def eliminate(rows, base):
    size = rows[0].shape[1]
    sub = lax.broadcasted_iota(jnp.int32, (SUB, size), 0)
    lane = lax.broadcasted_iota(jnp.int32, (SUB, size), 1)

    def row(x, k):
        return jnp.broadcast_to(x[k:k + 1, :], (SUB, size))

    for r in range(len(rows)):
        first = base + SUB * r
        cols = [[jnp.broadcast_to(x[:, first + j:first + j + 1], (SUB, size)) for j in range(SUB)] for x in rows]
        pivot, panel = list(cols[r]), rows[r]
        for k in range(0, SUB, 2):
            u, v = pivot[k], pivot[k + 1]
            a, c, b, d = row(u, k), row(u, k + 1), row(v, k), row(v, k + 1)
            inv = 1.0 / (a * d - b * c)

            def step(x, here=None, after=None):
                r0, r1 = row(x, k), row(x, k + 1)
                if here is not None:
                    r0 = jnp.where(here, 1.0, jnp.where(after, 0.0, r0))
                    r1 = jnp.where(after, 1.0, jnp.where(here, 0.0, r1))
                    x = jnp.where(here | after, 0.0, x)
                p0 = (d * r0 - b * r1) * inv
                p1 = (a * r1 - c * r0) * inv
                x = x - u * p0 - v * p1
                return jnp.where(sub == k, p0, jnp.where(sub == k + 1, p1, x))

            for j in range(k + 2, SUB):
                pivot[j] = step(pivot[j])
            panel = step(panel, lane == first + k, lane == first + k + 1)
        inside = (lane >= first) & (lane < first + SUB)
        heads = [row(panel, j) for j in range(SUB)]
        for i in range(len(rows)):
            if i != r:
                t = [cols[i][j] * heads[j] for j in range(SUB)]
                rows[i] = jnp.where(inside, 0.0, rows[i]) - (
                    ((t[0] + t[1]) + (t[2] + t[3])) + ((t[4] + t[5]) + (t[6] + t[7])))
        rows[r] = panel
    return jnp.concatenate(rows, axis=0)


def invert(c):
    size = c.shape[0]
    lane = lax.broadcasted_iota(jnp.int32, (1, size), 1)
    for base in range(0, size, PANEL):
        end = base + PANEL
        panel = eliminate([c[i:i + SUB, :] for i in range(base, end, SUB)], base)

        def framed(above, below):
            return jnp.concatenate([x for x in (above, panel, below) if x.shape[0]], axis=0)

        heads = framed(jnp.zeros((base, size), jnp.float32), jnp.zeros((size - end, size), jnp.float32))
        taken = jnp.dot(c, heads, precision=HIGHEST, preferred_element_type=jnp.float32)
        rest = jnp.where((lane >= base) & (lane < end), 0.0, c) - taken
        c = framed(rest[:base, :], rest[end:, :])
    return c


def split(x):
    high = x.astype(jnp.bfloat16)
    return high, (x - high.astype(jnp.float32)).astype(jnp.bfloat16)


def product(left, right):
    return lax.dot_general(left, right, (((0,), (0,)), ((), ())), preferred_element_type=jnp.float32)


def three(left_high, left_low, right_high, right_low):
    return product(left_high, right_high) + (product(left_high, right_low) + product(left_low, right_high))


def assemble_kernel(nq, nz, count_ref, window_ref, local_hbm, global_hbm, resid_hbm, weight_hbm,
                    out_ref, rhs_ref,
                    ls_ref, gs_ref, resid_ref, weight_ref, high, low, u_ref, u_high, u_low, x_high, x_low,
                    s_ref, own, recv, small, part, from_lo, from_hi, mirror, rsum, rrecv,
                    in_sem, send_sem, recv_sem, small_send, small_recv,
                    z_send, lo_sem, hi_sem, r_send, r_recv, m_send, m_recv):
    q = lax.axis_index("wide")
    z = lax.axis_index("narrow")
    slots, params = gs_ref.shape
    size = ls_ref.shape[1]
    groups = params // LANES
    cuts = LANES // CUT
    extra = cuts * nz
    chip, core = q // 2, lax.rem(q, 2)
    steps = 2 * nz

    def peer(step):
        return lax.rem(q + step, nq)

    wide = params // 4
    loads = [pltpu.make_async_copy(weight_hbm, weight_ref, in_sem.at[0]),
             pltpu.make_async_copy(resid_hbm, resid_ref, in_sem.at[1]),
             pltpu.make_async_copy(local_hbm, ls_ref, in_sem.at[2])]
    loads += [pltpu.make_async_copy(global_hbm.at[:, i * wide:(i + 1) * wide], gs_ref.at[:, i * wide:(i + 1) * wide],
                                    in_sem.at[3 + i]) for i in range(4)]
    for copy in loads:
        copy.start()
    barrier = pltpu.get_barrier_semaphore()
    for dz in range(nz):
        for step in range(nq):
            if dz or step:
                pl.semaphore_signal(barrier, inc=1, device_id=(peer(step), lax.rem(z + dz, nz)),
                                    device_id_type=MESH)
    for copy in loads:
        copy.wait()

    slot = lax.broadcasted_iota(jnp.int32, (1, slots), 1)
    root = jnp.sqrt(jnp.where(slot < count_ref[0], weight_ref[...], 0.0))
    root_col = jnp.broadcast_to(root, (LANES, slots)).T
    rs_col = jnp.broadcast_to(root * resid_ref[...], (LANES, slots)).T
    ls = ls_ref[...] * root_col
    ls_t = ls.T
    eye = (lax.broadcasted_iota(jnp.int32, (size, size), 0)
           == lax.broadcasted_iota(jnp.int32, (size, size), 1)).astype(jnp.float32)
    curv = jnp.dot(ls_t, ls, precision=HIGHEST, preferred_element_type=jnp.float32) + eye
    lr = jnp.sum(ls * rs_col, axis=0, keepdims=True)
    lr_col = jnp.broadcast_to(lr, (LANES, size)).T
    ls_high, ls_low = split(ls_t)
    for g in range(groups):
        cols = slice(g * LANES, (g + 1) * LANES)
        gs = gs_ref[:, cols] * root_col
        gs_high, gs_low = split(gs)
        high[:, cols], low[:, cols] = gs_high, gs_low
        own[g:g + 1, :] = jnp.sum(gs * rs_col, axis=0, keepdims=True)
    inverse = invert(curv)
    wide = 2 * LANES
    for g in range(0, params, wide):
        cols = slice(g, g + wide)
        coupling = (jnp.dot(ls_high, high[:, cols], preferred_element_type=jnp.float32)
                    + (jnp.dot(ls_high, low[:, cols], preferred_element_type=jnp.float32)
                       + jnp.dot(ls_low, high[:, cols], preferred_element_type=jnp.float32)))
        u_ref[:, cols] = coupling
        u_high[:, cols], u_low[:, cols] = split(coupling)
    for g in range(0, params, wide):
        cols = slice(g, g + wide)
        solved = jnp.dot(inverse, u_ref[:, cols], precision=HIGHEST, preferred_element_type=jnp.float32)
        x_high[:, cols], x_low[:, cols] = split(solved)
        for h in range(2):
            r = g // LANES + h
            own[r:r + 1, :] = own[r:r + 1, :] - jnp.sum(
                solved[:, h * LANES:(h + 1) * LANES] * lr_col, axis=0, keepdims=True)
    own[groups:, :] = (lax.broadcasted_iota(jnp.int32, (groups, LANES), 0) == window_ref[0]).astype(jnp.float32)

    orders = [sorted(range(nz), key=lambda a: (-abs(a - i), a if i >= nz // 2 else -a)) for i in range(nz)]

    def goal(k):
        a = jnp.int32(0)
        for i in range(nz):
            for j in range(nz):
                a = a + jnp.where((z == i) & (k == j), orders[i][j], 0)
        return a

    def place(a):
        k = jnp.int32(0)
        for i in range(nz):
            for j in range(nz):
                k = k + jnp.where((z == i) & (a == orders[i][j]), j, 0)
        return k

    late = cuts * place(chip) + cuts

    def chunk(i):
        plain = jnp.where(i > late, i - 1, i)
        k = jnp.minimum(plain // cuts, nz - 1)
        a = jnp.where(i == late, chip, goal(k))
        return jnp.where(i == late, extra, cuts * a + lax.rem(plain, cuts)), a

    def turn(col, a):
        return jnp.where(col // 2 <= a, lax.rem(col, 2), 1 - lax.rem(col, 2))

    def corner(t, col):
        a = jnp.minimum(t // cuts, nz - 1)
        row = (2 * a + turn(col, a)) * LANES + lax.rem(t, cuts) * CUT
        side = lax.rem(col, 2)
        row = jnp.where(t == extra, (2 * (col // 2) + 1) * LANES + side * CUT, row)
        left = jnp.where(t == extra, col - side, col) * LANES
        return pl.ds(pl.multiple_of(row, CUT), CUT), pl.ds(pl.multiple_of(left, LANES), LANES)

    def plane_copy(t, step):
        rows, cols = corner(t, peer(step))
        return pltpu.make_async_remote_copy(
            src_ref=s_ref.at[rows, cols], dst_ref=recv.at[nq - step, t],
            send_sem=send_sem.at[step, t], recv_sem=recv_sem.at[nq - step, t],
            device_id=(peer(step), z), device_id_type=MESH)

    def small_copy(step):
        return pltpu.make_async_remote_copy(
            src_ref=own, dst_ref=small.at[nq - step],
            send_sem=small_send.at[step], recv_sem=small_recv.at[nq - step],
            device_id=(peer(step), z), device_id_type=MESH)

    def up_copy(t):
        return pltpu.make_async_remote_copy(
            src_ref=part.at[t], dst_ref=from_lo.at[t], send_sem=z_send.at[t], recv_sem=lo_sem.at[t],
            device_id=(q, lax.min(z + 1, nz - 1)), device_id_type=MESH)

    def down_copy(t):
        return pltpu.make_async_remote_copy(
            src_ref=part.at[t], dst_ref=from_hi.at[t], send_sem=z_send.at[t], recv_sem=hi_sem.at[t],
            device_id=(q, lax.max(z - 1, 0)), device_id_type=MESH)

    def rhs_copy(step):
        return pltpu.make_async_remote_copy(
            src_ref=rsum, dst_ref=rrecv.at[nz - step],
            send_sem=r_send.at[step], recv_sem=r_recv.at[nz - step],
            device_id=(q, lax.rem(z + step, nz)), device_id_type=MESH)

    def mirror_copy(cut):
        return pltpu.make_async_remote_copy(
            src_ref=part.at[cuts * z + cut], dst_ref=mirror.at[cut], send_sem=m_send.at[cut], recv_sem=m_recv.at[cut],
            device_id=(2 * z + turn(q, z), chip), device_id_type=MESH)

    def swap_copy(cut):
        return pltpu.make_async_remote_copy(
            src_ref=part.at[extra], dst_ref=mirror.at[cut], send_sem=m_send.at[cut], recv_sem=m_recv.at[cut],
            device_id=(q + 1 - 2 * core, z), device_id_type=MESH)

    order = sorted(range(1, nq), key=lambda step: -min(step, nq - step))
    pl.semaphore_wait(barrier, nq * nz - 1)
    for step in order:
        small_copy(step).start()

    def send(i):
        a, h = goal(i // 2), lax.rem(i, 2)
        block = pl.ds(pl.multiple_of((2 * a + h) * LANES, LANES), LANES)
        s_ref[block, :] = (three(high[:, block], low[:, block], high[...], low[...])
                           - three(u_high[:, block], u_low[:, block], x_high[...], x_low[...]))
        for step in order:
            @pl.when(turn(peer(step), a) == h)
            def _(step=step):
                for cut in range(cuts):
                    plane_copy(cuts * a + cut, step).start()
        for step in order:
            @pl.when((peer(step) // 2 == a) & (h == 1))
            def _(step=step):
                plane_copy(extra, step).start()

    def gather(i):
        t, a = chunk(i)
        for step in order:
            plane_copy(t, nq - step).wait_recv()
        rows, cols = corner(t, q)
        recv[0, t] = s_ref[rows, cols]
        for w in range(NWIN):
            total = jnp.zeros((CUT, LANES), jnp.float32)
            for s in range(nq):
                total = total + small[s, groups + w:groups + w + 1, :] * recv[s, t]
            part[t, w] = total

        @pl.when((z == 0) & (a > z))
        def _():
            up_copy(t).start()

        @pl.when((z == nz - 1) & (a < z))
        def _():
            down_copy(t).start()

    def relay(i):
        t, a = chunk(i)

        @pl.when((z > 0) & (a > z))
        def _():
            up_copy(t).wait_recv()
            part[t] = part[t] + from_lo[t]
            up_copy(t).start()

        @pl.when((z < nz - 1) & (a < z))
        def _():
            down_copy(t).wait_recv()
            part[t] = part[t] + from_hi[t]
            down_copy(t).start()

    def finish(i):
        t, a = chunk(i)

        @pl.when(a == z)
        def _():
            @pl.when(z > 0)
            def _():
                up_copy(t).wait_recv()
                part[t] = part[t] + from_lo[t]

            @pl.when(z < nz - 1)
            def _():
                down_copy(t).wait_recv()
                part[t] = part[t] + from_hi[t]

            @pl.when(t == extra)
            def _():
                swap_copy(core).start()

            @pl.when(t != extra)
            def _():
                cut = lax.rem(t, cuts)

                @pl.when(chip != z)
                def _():
                    mirror_copy(cut).start()
                row = turn(q, z) * LANES + cut * CUT
                out_ref[:, pl.ds(pl.multiple_of(row, CUT), CUT), :] = part[t]

    def small_sums():
        small[0] = own[...]
        for step in range(1, nq):
            small_copy(nq - step).wait_recv()
        for w in range(NWIN):
            total = jnp.zeros((groups, LANES), jnp.float32)
            for s in range(nq):
                total = total + small[s, groups + w:groups + w + 1, :] * small[s, :groups, :]
            rsum[w] = total
        for step in range(1, nz):
            rhs_copy(step).start()

    lax.fori_loop(0, AHEAD, lambda i, carry: (send(i), carry)[1], 0)
    small_sums()

    def body(i, carry):
        @pl.when(i + AHEAD < steps)
        def _():
            send(i + AHEAD)

        @pl.when(i <= extra)
        def _():
            gather(i)

        @pl.when(i >= LAG)
        def _():
            relay(i - LAG)

        @pl.when(i <= extra)
        def _():
            finish(i)
        return carry

    lax.fori_loop(0, extra + 1 + LAG, body, 0)

    for step in range(1, nz):
        rhs_copy(nz - step).wait_recv()
    total = rsum[...]
    for step in range(1, nz):
        total = total + rrecv[step]
    rrecv[0] = total
    for w in range(NWIN):
        for h in range(2):
            rhs_ref[w:w + 1, h * LANES:(h + 1) * LANES] = rrecv[0, w, pl.ds(2 * z + h, 1), :]

    @pl.when(chip != z)
    def _():
        for cut in range(cuts):
            mirror_copy(cut).wait_recv()
        row = (1 - turn(q, z)) * LANES
        for w in range(NWIN):
            block = jnp.concatenate([mirror[cut, w] for cut in range(cuts)], axis=0)
            out_ref[w, pl.ds(pl.multiple_of(row, LANES), LANES), :] = block.T

    for side in range(2):
        @pl.when((chip == z) & (core == side))
        def _(side=side):
            swap_copy(1 - side).wait_recv()
            for w in range(NWIN):
                pieces = [part[extra, w] if cut == side else mirror[cut, w] for cut in range(cuts)]
                block = jnp.concatenate(pieces, axis=0)
                out_ref[w, (1 - side) * LANES:(2 - side) * LANES, :] = block.T if side else block

    for step in range(1, nq):
        small_copy(step).wait_send()
    for step in range(1, nz):
        rhs_copy(step).wait_send()

    @pl.when(chip != z)
    def _():
        for cut in range(cuts):
            mirror_copy(cut).wait_send()

    @pl.when(chip == z)
    def _():
        swap_copy(core).wait_send()

    def drain(t, carry):
        for step in range(1, nq):
            plane_copy(t, step).wait_send()
        a = jnp.where(t == extra, chip, t // cuts)

        @pl.when(a != z)
        def _():
            up_copy(t).wait_send()
        return carry

    lax.fori_loop(0, extra + 1, drain, 0)


def assemble(nq, nz, count, window, local_b, global_b, resid, weight):
    slots, params = global_b.shape
    size = local_b.shape[1]
    groups = params // LANES
    cuts = LANES // CUT
    chunks = cuts * nz + 1
    smem = pl.BlockSpec(memory_space=pltpu.SMEM)
    hbm = pl.BlockSpec(memory_space=pltpu.HBM)
    vmem = pl.BlockSpec(memory_space=pltpu.VMEM)
    f32, bf16 = jnp.float32, jnp.bfloat16
    block = pltpu.VMEM((chunks, NWIN, CUT, LANES), f32)
    dma = pltpu.SemaphoreType.DMA
    return pl.pallas_call(
        functools.partial(assemble_kernel, nq, nz),
        out_shape=(jax.ShapeDtypeStruct((NWIN, params // nz, LANES), f32),
                   jax.ShapeDtypeStruct((NWIN, params // nz), f32)),
        in_specs=[smem, smem, hbm, hbm, hbm, hbm],
        out_specs=(vmem, vmem),
        scratch_shapes=[
            pltpu.VMEM((slots, size), f32), pltpu.VMEM((slots, params), f32),
            pltpu.VMEM((1, slots), f32), pltpu.VMEM((1, slots), f32),
            pltpu.VMEM((slots, params), bf16), pltpu.VMEM((slots, params), bf16),
            pltpu.VMEM((size, params), f32),
            pltpu.VMEM((size, params), bf16), pltpu.VMEM((size, params), bf16),
            pltpu.VMEM((size, params), bf16), pltpu.VMEM((size, params), bf16),
            pltpu.VMEM((params, params), f32),
            pltpu.VMEM((2 * groups, LANES), f32),
            pltpu.VMEM((nq, chunks, CUT, LANES), f32),
            pltpu.VMEM((nq, 2 * groups, LANES), f32),
            block, block, block,
            pltpu.VMEM((cuts, NWIN, CUT, LANES), f32),
            pltpu.VMEM((NWIN, groups, LANES), f32),
            pltpu.VMEM((nz, NWIN, groups, LANES), f32),
            dma((7,)), dma((nq, chunks)), dma((nq, chunks)), dma((nq,)), dma((nq,)),
            dma((chunks,)), dma((chunks,)), dma((chunks,)), dma((nz,)), dma((nz,)),
            dma((cuts,)), dma((cuts,)),
        ],
        compiler_params=pltpu.CompilerParams(
            collective_id=0, has_side_effects=True, vmem_limit_bytes=48 * 1024 * 1024),
        name="assemble",
    )(count, window, local_b, global_b, resid, weight)


def reduced_bundle(local_b, global_b, resid_b, weight_b, count):
    measure_slot, local_param = local_b.shape
    slots = jnp.arange(measure_slot, dtype=jnp.int32)
    live = jnp.where(slots < count, weight_b, jnp.float32(0.0))
    root = jnp.sqrt(live)[:, None]
    ls = local_b * root
    gs = global_b * root
    rs = resid_b[:, None] * root
    curv = tdot(ls, ls) + jnp.eye(local_param, dtype=jnp.float32)
    coupling = tdot(ls, gs)
    lr = tdot(ls, rs)
    gr = tdot(gs, rs)[:, 0]
    factor = jnp.linalg.cholesky(curv)
    solved_all = jax.scipy.linalg.cho_solve((factor, True), jnp.concatenate([coupling, lr], axis=1))
    solved, solved_rhs = solved_all[:, :-1], solved_all[:, -1:]
    schur = tdot(gs, gs, HIGH) - tdot(coupling, solved, HIGH)
    reduced = gr - tdot(coupling, solved_rhs)[:, 0]
    return schur, reduced


def on_device(local_slopes, global_slopes, residuals, weights, track_slot_count, windows):
    nq, nz = lax.axis_size("wide"), lax.axis_size("narrow")
    slots, params = global_slopes.shape[1:]
    owned = params // nz
    z = lax.axis_index("narrow")
    if params // nq == LANES and local_slopes.shape[2] == LANES and nq == 2 * nz and nz > 1:
        return assemble(nq, nz, track_slot_count, windows, local_slopes[0], global_slopes[0], residuals, weights)
    schur, reduced = reduced_bundle(
        local_slopes[0], global_slopes[0], residuals[0], weights[0], track_slot_count[0])
    picks = (windows[0] == jnp.arange(NWIN, dtype=jnp.int32)).astype(jnp.float32)
    rhs_whole = lax.psum(picks[:, None] * reduced[None], ("wide", "narrow"))
    normal_rhs = lax.dynamic_slice_in_dim(rhs_whole, z * owned, owned, 1)
    received = lax.all_to_all(schur[None], "wide", split_axis=2, concat_axis=0, tiled=True)
    all_picks = lax.all_gather(picks, "wide", axis=0)
    partial_value = jnp.einsum("bw,bij->wij", all_picks, received, precision=HIGHEST,
                               preferred_element_type=jnp.float32)
    return lax.psum_scatter(partial_value, "narrow", scatter_dimension=1, tiled=True), normal_rhs


def solution(mesh):
    in_specs = (
        P(("wide", "narrow"), None, None),
        P(("wide", "narrow"), None, None),
        P(("wide", "narrow"), None),
        P(("wide", "narrow"), None),
        P(("wide", "narrow")),
        P(("wide", "narrow")),
    )
    out_specs = (P(None, "narrow", "wide"), P(None, "narrow"))
    return jax.shard_map(
        on_device, mesh=mesh, in_specs=in_specs, out_specs=out_specs, check_vma=False
    )
```

```python
import functools
import jax
import jax.numpy as jnp
from jax import lax
from jax.experimental import pallas as pl
from jax.experimental.pallas import tpu as pltpu
from jax.sharding import PartitionSpec as P

WINDOW_PARAMS = 1024
NWIN = 4
LANES = 128
SUB = 8
PANEL = 32
CUT = 64
AHEAD = 4
LAG = 1
SETTLE = 3
MESH = pl.DeviceIdType.MESH
HIGHEST = lax.Precision.HIGHEST
HIGH = lax.Precision.HIGH


def tdot(left, right, precision=HIGHEST):
    return lax.dot_general(
        left,
        right,
        (((0,), (0,)), ((), ())),
        precision=precision,
        preferred_element_type=jnp.float32,
    )


def eliminate(rows, base):
    size = rows[0].shape[1]
    sub = lax.broadcasted_iota(jnp.int32, (SUB, size), 0)
    lane = lax.broadcasted_iota(jnp.int32, (SUB, size), 1)

    def row(x, k):
        return jnp.broadcast_to(x[k:k + 1, :], (SUB, size))

    for r in range(len(rows)):
        first = base + SUB * r
        cols = [[jnp.broadcast_to(x[:, first + j:first + j + 1], (SUB, size)) for j in range(SUB)] for x in rows]
        pivot, panel = list(cols[r]), rows[r]
        for k in range(0, SUB, 2):
            u, v = pivot[k], pivot[k + 1]
            a, c, b, d = row(u, k), row(u, k + 1), row(v, k), row(v, k + 1)
            inv = 1.0 / (a * d - b * c)

            def step(x, here=None, after=None):
                r0, r1 = row(x, k), row(x, k + 1)
                if here is not None:
                    r0 = jnp.where(here, 1.0, jnp.where(after, 0.0, r0))
                    r1 = jnp.where(after, 1.0, jnp.where(here, 0.0, r1))
                    x = jnp.where(here | after, 0.0, x)
                p0 = (d * r0 - b * r1) * inv
                p1 = (a * r1 - c * r0) * inv
                x = x - u * p0 - v * p1
                return jnp.where(sub == k, p0, jnp.where(sub == k + 1, p1, x))

            for j in range(k + 2, SUB):
                pivot[j] = step(pivot[j])
            panel = step(panel, lane == first + k, lane == first + k + 1)
        inside = (lane >= first) & (lane < first + SUB)
        heads = [row(panel, j) for j in range(SUB)]
        for i in range(len(rows)):
            if i != r:
                t = [cols[i][j] * heads[j] for j in range(SUB)]
                rows[i] = jnp.where(inside, 0.0, rows[i]) - (
                    ((t[0] + t[1]) + (t[2] + t[3])) + ((t[4] + t[5]) + (t[6] + t[7])))
        rows[r] = panel
    return jnp.concatenate(rows, axis=0)


def invert_panel(c, base):
    size = c.shape[0]
    lane = lax.broadcasted_iota(jnp.int32, (1, size), 1)
    end = base + PANEL
    panel = eliminate([c[i:i + SUB, :] for i in range(base, end, SUB)], base)

    def framed(above, below):
        return jnp.concatenate([x for x in (above, panel, below) if x.shape[0]], axis=0)

    heads = framed(jnp.zeros((base, size), jnp.float32), jnp.zeros((size - end, size), jnp.float32))
    taken = jnp.dot(c, heads, precision=HIGHEST, preferred_element_type=jnp.float32)
    rest = jnp.where((lane >= base) & (lane < end), 0.0, c) - taken
    return framed(rest[:base, :], rest[end:, :])


def split(x):
    high = x.astype(jnp.bfloat16)
    return high, (x - high.astype(jnp.float32)).astype(jnp.bfloat16)


def product(left, right):
    return lax.dot_general(left, right, (((0,), (0,)), ((), ())), preferred_element_type=jnp.float32)


def three(left_high, left_low, right_high, right_low):
    return product(left_high, right_high) + (product(left_high, right_low) + product(left_low, right_high))


def assemble_kernel(nq, nz, count_ref, window_ref, local_hbm, global_hbm, resid_hbm, weight_hbm,
                    out_ref, rhs_ref,
                    ls_ref, gs_ref, resid_ref, weight_ref, high, low, u_ref, u_high, u_low, x_high, x_low,
                    s_ref, own, recv, small, part, from_lo, from_hi, mirror, hold, rsum, rrecv,
                    in_sem, send_sem, recv_sem, small_send, small_recv,
                    z_send, lo_sem, hi_sem, r_send, r_recv, m_send, m_recv, h_send, h_recv):
    q = lax.axis_index("wide")
    z = lax.axis_index("narrow")
    slots, params = gs_ref.shape
    size = ls_ref.shape[1]
    groups = params // LANES
    cuts = LANES // CUT
    extra = cuts * nz
    chip, core = q // 2, lax.rem(q, 2)
    steps = 2 * nz

    def peer(step):
        return lax.rem(q + step, nq)

    wide = params // 4
    loads = [pltpu.make_async_copy(weight_hbm, weight_ref, in_sem.at[0]),
             pltpu.make_async_copy(resid_hbm, resid_ref, in_sem.at[1]),
             pltpu.make_async_copy(local_hbm, ls_ref, in_sem.at[2])]
    loads += [pltpu.make_async_copy(global_hbm.at[:, i * wide:(i + 1) * wide], gs_ref.at[:, i * wide:(i + 1) * wide],
                                    in_sem.at[3 + i]) for i in range(4)]
    for copy in loads:
        copy.start()
    barrier = pltpu.get_barrier_semaphore()
    for dz in range(nz):
        for step in range(nq):
            if dz or step:
                pl.semaphore_signal(barrier, inc=1, device_id=(peer(step), lax.rem(z + dz, nz)),
                                    device_id_type=MESH)
    for copy in loads[:3]:
        copy.wait()

    slot = lax.broadcasted_iota(jnp.int32, (1, slots), 1)
    root = jnp.sqrt(jnp.where(slot < count_ref[0], weight_ref[...], 0.0))
    root_col = jnp.broadcast_to(root, (LANES, slots)).T
    rs_col = jnp.broadcast_to(root * resid_ref[...], (LANES, slots)).T
    ls = ls_ref[...] * root_col
    ls_t = ls.T
    eye = (lax.broadcasted_iota(jnp.int32, (size, size), 0)
           == lax.broadcasted_iota(jnp.int32, (size, size), 1)).astype(jnp.float32)
    curv = jnp.dot(ls_t, ls, precision=HIGHEST, preferred_element_type=jnp.float32) + eye
    lr = jnp.sum(ls * rs_col, axis=0, keepdims=True)
    lr_col = jnp.broadcast_to(lr, (LANES, size)).T
    ls_high, ls_low = split(ls_t)
    wide = 2 * LANES

    def couple():
        for g in range(groups):
            cols = slice(g * LANES, (g + 1) * LANES)
            gs = gs_ref[:, cols] * root_col
            high[:, cols], low[:, cols] = split(gs)
            own[g:g + 1, :] = jnp.sum(gs * rs_col, axis=0, keepdims=True)
        for g in range(0, params, wide):
            cols = slice(g, g + wide)
            coupling = (jnp.dot(ls_high, high[:, cols], preferred_element_type=jnp.float32)
                        + (jnp.dot(ls_high, low[:, cols], preferred_element_type=jnp.float32)
                           + jnp.dot(ls_low, high[:, cols], preferred_element_type=jnp.float32)))
            u_ref[:, cols] = coupling
            u_high[:, cols], u_low[:, cols] = split(coupling)

    inverse = invert_panel(curv, 0)
    for copy in loads[3:]:
        copy.wait()
    couple()
    for base in range(PANEL, size, PANEL):
        inverse = invert_panel(inverse, base)

    for g in range(0, params, wide):
        cols = slice(g, g + wide)
        solved = jnp.dot(inverse, u_ref[:, cols], precision=HIGHEST, preferred_element_type=jnp.float32)
        x_high[:, cols], x_low[:, cols] = split(solved)
        for h in range(2):
            r = g // LANES + h
            own[r:r + 1, :] = own[r:r + 1, :] - jnp.sum(
                solved[:, h * LANES:(h + 1) * LANES] * lr_col, axis=0, keepdims=True)
    own[groups:, :] = (lax.broadcasted_iota(jnp.int32, (groups, LANES), 0) == window_ref[0]).astype(jnp.float32)

    orders = [sorted(range(nz), key=lambda a: (min(a, nz - 1 - a), -abs(a - i))) for i in range(nz)]

    def goal(k):
        a = jnp.int32(0)
        for i in range(nz):
            for j in range(nz):
                a = a + jnp.where((z == i) & (k == j), orders[i][j], 0)
        return a

    def place(a):
        k = jnp.int32(0)
        for i in range(nz):
            for j in range(nz):
                k = k + jnp.where((z == i) & (a == orders[i][j]), j, 0)
        return k

    late = cuts * place(chip) + cuts

    def final(i):
        plain = jnp.where(i > late, i - 1, i)
        return jnp.where(i == late, place(chip), jnp.minimum(plain // cuts, nz - 1)) == nz - 1

    def chunk(i):
        plain = jnp.where(i > late, i - 1, i)
        k = jnp.minimum(plain // cuts, nz - 1)
        a = jnp.where(i == late, chip, goal(k))
        return jnp.where(i == late, extra, cuts * a + lax.rem(plain, cuts)), a

    def turn(col, a):
        return jnp.where(col // 2 <= a, lax.rem(col, 2), 1 - lax.rem(col, 2))

    def corner(t, col):
        a = jnp.minimum(t // cuts, nz - 1)
        row = (2 * a + turn(col, a)) * LANES + lax.rem(t, cuts) * CUT
        side = lax.rem(col, 2)
        row = jnp.where(t == extra, (2 * (col // 2) + 1) * LANES + side * CUT, row)
        left = jnp.where(t == extra, col - side, col) * LANES
        return pl.ds(pl.multiple_of(row, CUT), CUT), pl.ds(pl.multiple_of(left, LANES), LANES)

    def plane_copy(t, step):
        rows, cols = corner(t, peer(step))
        return pltpu.make_async_remote_copy(
            src_ref=s_ref.at[rows, cols], dst_ref=recv.at[nq - step, t],
            send_sem=send_sem.at[step, t], recv_sem=recv_sem.at[nq - step, t],
            device_id=(peer(step), z), device_id_type=MESH)

    def small_copy(step):
        return pltpu.make_async_remote_copy(
            src_ref=own, dst_ref=small.at[nq - step],
            send_sem=small_send.at[step], recv_sem=small_recv.at[nq - step],
            device_id=(peer(step), z), device_id_type=MESH)

    def up_copy(t):
        return pltpu.make_async_remote_copy(
            src_ref=part.at[t], dst_ref=from_lo.at[t], send_sem=z_send.at[t], recv_sem=lo_sem.at[t],
            device_id=(q, lax.min(z + 1, nz - 1)), device_id_type=MESH)

    def down_copy(t):
        return pltpu.make_async_remote_copy(
            src_ref=part.at[t], dst_ref=from_hi.at[t], send_sem=z_send.at[t], recv_sem=hi_sem.at[t],
            device_id=(q, lax.max(z - 1, 0)), device_id_type=MESH)

    def rhs_copy(step):
        return pltpu.make_async_remote_copy(
            src_ref=rsum, dst_ref=rrecv.at[nz - step],
            send_sem=r_send.at[step], recv_sem=r_recv.at[nz - step],
            device_id=(q, lax.rem(z + step, nz)), device_id_type=MESH)

    def mirror_copy(cut):
        return pltpu.make_async_remote_copy(
            src_ref=part.at[cuts * z + cut], dst_ref=mirror.at[cut], send_sem=m_send.at[cut], recv_sem=m_recv.at[cut],
            device_id=(2 * z + turn(q, z), chip), device_id_type=MESH)

    def hold_copy():
        return pltpu.make_async_remote_copy(
            src_ref=part.at[cuts * z], dst_ref=hold.at[chip], send_sem=m_send.at[0], recv_sem=h_recv.at[chip],
            device_id=(2 * z + turn(q, z), z), device_id_type=MESH)

    def forward_copy(a):
        return pltpu.make_async_remote_copy(
            src_ref=hold.at[a], dst_ref=mirror.at[0], send_sem=h_send.at[a], recv_sem=m_recv.at[0],
            device_id=(q, a), device_id_type=MESH)

    def arrived(a):
        return pltpu.make_async_remote_copy(
            src_ref=part.at[cuts * z], dst_ref=hold.at[a], send_sem=m_send.at[0], recv_sem=h_recv.at[a],
            device_id=(2 * z + turn(q, z), z), device_id_type=MESH)

    def forward(a):
        @pl.when((chip == z) & (z != a))
        def _():
            arrived(a).wait_recv()
            forward_copy(a).start()

    def swap_copy(cut):
        return pltpu.make_async_remote_copy(
            src_ref=part.at[extra], dst_ref=mirror.at[cut], send_sem=m_send.at[cut], recv_sem=m_recv.at[cut],
            device_id=(q + 1 - 2 * core, z), device_id_type=MESH)

    order = sorted(range(1, nq), key=lambda step: -min(step, nq - step))
    pl.semaphore_wait(barrier, nq * nz - 1)
    for step in order:
        small_copy(step).start()

    def send(i):
        a, h = goal(i // 2), lax.rem(i, 2)
        block = pl.ds(pl.multiple_of((2 * a + h) * LANES, LANES), LANES)
        s_ref[block, :] = (three(high[:, block], low[:, block], high[...], low[...])
                           - three(u_high[:, block], u_low[:, block], x_high[...], x_low[...]))
        for step in order:
            @pl.when(turn(peer(step), a) == h)
            def _(step=step):
                for cut in range(cuts):
                    plane_copy(cuts * a + cut, step).start()
        for step in order:
            @pl.when((peer(step) // 2 == a) & (h == 1))
            def _(step=step):
                plane_copy(extra, step).start()

    def gather(i):
        t, a = chunk(i)
        for step in order:
            plane_copy(t, nq - step).wait_recv()
        rows, cols = corner(t, q)
        recv[0, t] = s_ref[rows, cols]
        for w in range(NWIN):
            total = jnp.zeros((CUT, LANES), jnp.float32)
            for s in range(nq):
                total = total + small[s, groups + w:groups + w + 1, :] * recv[s, t]
            part[t, w] = total

        @pl.when((z == 0) & (a > z))
        def _():
            up_copy(t).start()

        @pl.when((z == nz - 1) & (a < z))
        def _():
            down_copy(t).start()

    def relay(i):
        t, a = chunk(i)

        @pl.when((z > 0) & (a > z))
        def _():
            up_copy(t).wait_recv()
            part[t] = part[t] + from_lo[t]
            up_copy(t).start()

        @pl.when((z < nz - 1) & (a < z))
        def _():
            down_copy(t).wait_recv()
            part[t] = part[t] + from_hi[t]
            down_copy(t).start()

    def finish(i):
        t, a = chunk(i)

        @pl.when(a == z)
        def _():
            @pl.when(z > 0)
            def _():
                up_copy(t).wait_recv()
                part[t] = part[t] + from_lo[t]

            @pl.when(z < nz - 1)
            def _():
                down_copy(t).wait_recv()
                part[t] = part[t] + from_hi[t]

            @pl.when(t == extra)
            def _():
                swap_copy(core).start()

            @pl.when(t != extra)
            def _():
                cut = lax.rem(t, cuts)

                @pl.when((chip != z) & (cut == 0))
                def _():
                    hold_copy().start()

                @pl.when((chip != z) & (cut != 0))
                def _():
                    mirror_copy(cut).start()
                row = turn(q, z) * LANES + cut * CUT
                out_ref[:, pl.ds(pl.multiple_of(row, CUT), CUT), :] = part[t]

    def small_sums():
        small[0] = own[...]
        for step in range(1, nq):
            small_copy(nq - step).wait_recv()
        for w in range(NWIN):
            total = jnp.zeros((groups, LANES), jnp.float32)
            for s in range(nq):
                total = total + small[s, groups + w:groups + w + 1, :] * small[s, :groups, :]
            rsum[w] = total
        for step in range(1, nz):
            rhs_copy(step).start()

    lax.fori_loop(0, AHEAD, lambda i, carry: (send(i), carry)[1], 0)
    small_sums()

    def body(i, carry):
        @pl.when(i + AHEAD < steps)
        def _():
            send(i + AHEAD)

        @pl.when(i <= extra)
        def _():
            gather(i)

        @pl.when(i >= LAG)
        def _():
            relay(i - LAG)

        @pl.when((i >= SETTLE) & jnp.logical_not(final(i - SETTLE)))
        def _():
            finish(i - SETTLE)

        @pl.when((i <= extra) & final(i))
        def _():
            finish(i)

        for g in range(nz // 2 - 1):
            @pl.when(i == 2 * cuts * (g + 1) + SETTLE + 2)
            def _(g=g):
                forward(g)
                forward(nz - 1 - g)
        return carry

    lax.fori_loop(0, extra + 1 + LAG, body, 0)
    for a in range(nz // 2 - 1, nz - nz // 2 + 1):
        forward(a)

    for step in range(1, nz):
        rhs_copy(nz - step).wait_recv()
    total = rsum[...]
    for step in range(1, nz):
        total = total + rrecv[step]
    rrecv[0] = total
    for w in range(NWIN):
        for h in range(2):
            rhs_ref[w:w + 1, h * LANES:(h + 1) * LANES] = rrecv[0, w, pl.ds(2 * z + h, 1), :]

    @pl.when(chip != z)
    def _():
        for cut in range(cuts):
            mirror_copy(cut).wait_recv()
        row = (1 - turn(q, z)) * LANES
        for w in range(NWIN):
            block = jnp.concatenate([mirror[cut, w] for cut in range(cuts)], axis=0)
            out_ref[w, pl.ds(pl.multiple_of(row, LANES), LANES), :] = block.T

    for side in range(2):
        @pl.when((chip == z) & (core == side))
        def _(side=side):
            swap_copy(1 - side).wait_recv()
            for w in range(NWIN):
                pieces = [part[extra, w] if cut == side else mirror[cut, w] for cut in range(cuts)]
                block = jnp.concatenate(pieces, axis=0)
                out_ref[w, (1 - side) * LANES:(2 - side) * LANES, :] = block.T if side else block

    for step in range(1, nq):
        small_copy(step).wait_send()
    for step in range(1, nz):
        rhs_copy(step).wait_send()

    @pl.when(chip != z)
    def _():
        for cut in range(cuts):
            mirror_copy(cut).wait_send()

    @pl.when(chip == z)
    def _():
        swap_copy(core).wait_send()
        for a in range(nz):
            @pl.when(z != a)
            def _(a=a):
                forward_copy(a).wait_send()

    def drain(t, carry):
        for step in range(1, nq):
            plane_copy(t, step).wait_send()
        a = jnp.where(t == extra, chip, t // cuts)

        @pl.when(a != z)
        def _():
            up_copy(t).wait_send()
        return carry

    lax.fori_loop(0, extra + 1, drain, 0)


def assemble(nq, nz, count, window, local_b, global_b, resid, weight):
    slots, params = global_b.shape
    size = local_b.shape[1]
    groups = params // LANES
    cuts = LANES // CUT
    chunks = cuts * nz + 1
    smem = pl.BlockSpec(memory_space=pltpu.SMEM)
    hbm = pl.BlockSpec(memory_space=pltpu.HBM)
    vmem = pl.BlockSpec(memory_space=pltpu.VMEM)
    f32, bf16 = jnp.float32, jnp.bfloat16
    block = pltpu.VMEM((chunks, NWIN, CUT, LANES), f32)
    dma = pltpu.SemaphoreType.DMA
    return pl.pallas_call(
        functools.partial(assemble_kernel, nq, nz),
        out_shape=(jax.ShapeDtypeStruct((NWIN, params // nz, LANES), f32),
                   jax.ShapeDtypeStruct((NWIN, params // nz), f32)),
        in_specs=[smem] * 2 + [hbm] * 4,
        out_specs=(vmem, vmem),
        scratch_shapes=[
            pltpu.VMEM((slots, size), f32), pltpu.VMEM((slots, params), f32),
            pltpu.VMEM((1, slots), f32), pltpu.VMEM((1, slots), f32),
            pltpu.VMEM((slots, params), bf16), pltpu.VMEM((slots, params), bf16),
            pltpu.VMEM((size, params), f32),
            pltpu.VMEM((size, params), bf16), pltpu.VMEM((size, params), bf16),
            pltpu.VMEM((size, params), bf16), pltpu.VMEM((size, params), bf16),
            pltpu.VMEM((params, params), f32),
            pltpu.VMEM((2 * groups, LANES), f32),
            pltpu.VMEM((nq, chunks, CUT, LANES), f32),
            pltpu.VMEM((nq, 2 * groups, LANES), f32),
            block, block, block,
            pltpu.VMEM((cuts, NWIN, CUT, LANES), f32), pltpu.VMEM((nz, NWIN, CUT, LANES), f32),
            pltpu.VMEM((NWIN, groups, LANES), f32),
            pltpu.VMEM((nz, NWIN, groups, LANES), f32),
            dma((7,)), dma((nq, chunks)), dma((nq, chunks)), dma((nq,)), dma((nq,)),
            dma((chunks,)), dma((chunks,)), dma((chunks,)), dma((nz,)), dma((nz,)),
            dma((cuts,)), dma((cuts,)), dma((nz,)), dma((nz,)),
        ],
        compiler_params=pltpu.CompilerParams(
            collective_id=0, has_side_effects=True, vmem_limit_bytes=48 * 1024 * 1024),
        name="assemble",
    )(count, window, *(pltpu.with_memory_space_constraint(x, pltpu.HBM) for x in (local_b, global_b, resid, weight)))


def reduced_bundle(local_b, global_b, resid_b, weight_b, count):
    measure_slot, local_param = local_b.shape
    slots = jnp.arange(measure_slot, dtype=jnp.int32)
    live = jnp.where(slots < count, weight_b, jnp.float32(0.0))
    root = jnp.sqrt(live)[:, None]
    ls = local_b * root
    gs = global_b * root
    rs = resid_b[:, None] * root
    curv = tdot(ls, ls) + jnp.eye(local_param, dtype=jnp.float32)
    coupling = tdot(ls, gs)
    lr = tdot(ls, rs)
    gr = tdot(gs, rs)[:, 0]
    factor = jnp.linalg.cholesky(curv)
    solved_all = jax.scipy.linalg.cho_solve((factor, True), jnp.concatenate([coupling, lr], axis=1))
    solved, solved_rhs = solved_all[:, :-1], solved_all[:, -1:]
    schur = tdot(gs, gs, HIGH) - tdot(coupling, solved, HIGH)
    reduced = gr - tdot(coupling, solved_rhs)[:, 0]
    return schur, reduced


def on_device(local_slopes, global_slopes, residuals, weights, track_slot_count, windows):
    nq, nz = lax.axis_size("wide"), lax.axis_size("narrow")
    slots, params = global_slopes.shape[1:]
    owned = params // nz
    z = lax.axis_index("narrow")
    if params // nq == LANES and local_slopes.shape[2] == LANES and nq == 2 * nz and nz > 1:
        return assemble(nq, nz, track_slot_count, windows, local_slopes[0], global_slopes[0], residuals, weights)
    schur, reduced = reduced_bundle(
        local_slopes[0], global_slopes[0], residuals[0], weights[0], track_slot_count[0])
    picks = (windows[0] == jnp.arange(NWIN, dtype=jnp.int32)).astype(jnp.float32)
    rhs_whole = lax.psum(picks[:, None] * reduced[None], ("wide", "narrow"))
    normal_rhs = lax.dynamic_slice_in_dim(rhs_whole, z * owned, owned, 1)
    received = lax.all_to_all(schur[None], "wide", split_axis=2, concat_axis=0, tiled=True)
    all_picks = lax.all_gather(picks, "wide", axis=0)
    partial_value = jnp.einsum("bw,bij->wij", all_picks, received, precision=HIGHEST,
                               preferred_element_type=jnp.float32)
    return lax.psum_scatter(partial_value, "narrow", scatter_dimension=1, tiled=True), normal_rhs


def solution(mesh):
    in_specs = (
        P(("wide", "narrow"), None, None),
        P(("wide", "narrow"), None, None),
        P(("wide", "narrow"), None),
        P(("wide", "narrow"), None),
        P(("wide", "narrow")),
        P(("wide", "narrow")),
    )
    out_specs = (P(None, "narrow", "wide"), P(None, "narrow"))
    return jax.shard_map(
        on_device, mesh=mesh, in_specs=in_specs, out_specs=out_specs, check_vma=False
    )
```

```python
import functools
import jax
import jax.numpy as jnp
from jax import lax
from jax.experimental import pallas as pl
from jax.experimental.pallas import tpu as pltpu
from jax.sharding import PartitionSpec as P

WINDOW_PARAMS = 1024
NWIN = 4
LANES = 128
SUB = 8
PANEL = 32
CUT = 64
AHEAD = 4
LAG = 1
SETTLE = 3
HOP = 3
MIRROR = -0.8
MESH = pl.DeviceIdType.MESH
HIGHEST = lax.Precision.HIGHEST
HIGH = lax.Precision.HIGH


def tdot(left, right, precision=HIGHEST):
    return lax.dot_general(
        left,
        right,
        (((0,), (0,)), ((), ())),
        precision=precision,
        preferred_element_type=jnp.float32,
    )


def eliminate(rows, base):
    size = rows[0].shape[1]
    sub = lax.broadcasted_iota(jnp.int32, (SUB, size), 0)
    lane = lax.broadcasted_iota(jnp.int32, (SUB, size), 1)

    def row(x, k):
        return jnp.broadcast_to(x[k:k + 1, :], (SUB, size))

    for r in range(len(rows)):
        first = base + SUB * r
        cols = [[jnp.broadcast_to(x[:, first + j:first + j + 1], (SUB, size)) for j in range(SUB)] for x in rows]
        pivot, panel = list(cols[r]), rows[r]
        for k in range(0, SUB, 2):
            u, v = pivot[k], pivot[k + 1]
            a, c, b, d = row(u, k), row(u, k + 1), row(v, k), row(v, k + 1)
            inv = 1.0 / (a * d - b * c)

            def step(x, here=None, after=None):
                r0, r1 = row(x, k), row(x, k + 1)
                if here is not None:
                    r0 = jnp.where(here, 1.0, jnp.where(after, 0.0, r0))
                    r1 = jnp.where(after, 1.0, jnp.where(here, 0.0, r1))
                    x = jnp.where(here | after, 0.0, x)
                p0 = (d * r0 - b * r1) * inv
                p1 = (a * r1 - c * r0) * inv
                x = x - u * p0 - v * p1
                return jnp.where(sub == k, p0, jnp.where(sub == k + 1, p1, x))

            for j in range(k + 2, SUB):
                pivot[j] = step(pivot[j])
            panel = step(panel, lane == first + k, lane == first + k + 1)
        inside = (lane >= first) & (lane < first + SUB)
        heads = [row(panel, j) for j in range(SUB)]
        for i in range(len(rows)):
            if i != r:
                t = [cols[i][j] * heads[j] for j in range(SUB)]
                rows[i] = jnp.where(inside, 0.0, rows[i]) - (
                    ((t[0] + t[1]) + (t[2] + t[3])) + ((t[4] + t[5]) + (t[6] + t[7])))
        rows[r] = panel
    return jnp.concatenate(rows, axis=0)


def invert_panel(c, base):
    size = c.shape[0]
    lane = lax.broadcasted_iota(jnp.int32, (1, size), 1)
    end = base + PANEL
    panel = eliminate([c[i:i + SUB, :] for i in range(base, end, SUB)], base)

    def framed(above, below):
        return jnp.concatenate([x for x in (above, panel, below) if x.shape[0]], axis=0)

    heads = framed(jnp.zeros((base, size), jnp.float32), jnp.zeros((size - end, size), jnp.float32))
    taken = jnp.dot(c, heads, precision=HIGHEST, preferred_element_type=jnp.float32)
    rest = jnp.where((lane >= base) & (lane < end), 0.0, c) - taken
    return framed(rest[:base, :], rest[end:, :])


def split(x):
    high = x.astype(jnp.bfloat16)
    return high, (x - high.astype(jnp.float32)).astype(jnp.bfloat16)


def product(left, right):
    return lax.dot_general(left, right, (((0,), (0,)), ((), ())), preferred_element_type=jnp.float32)


def three(left_high, left_low, right_high, right_low):
    return product(left_high, right_high) + (product(left_high, right_low) + product(left_low, right_high))


def assemble_kernel(nq, nz, count_ref, window_ref, local_hbm, global_hbm, resid_hbm, weight_hbm,
                    out_ref, rhs_ref,
                    ls_ref, gs_ref, resid_ref, weight_ref, high, low, u_ref, u_high, u_low, x_high, x_low,
                    s_ref, own, recv, small, part, from_lo, from_hi, mirror, hold, rsum, rrecv,
                    in_sem, send_sem, recv_sem, small_send, small_recv,
                    z_send, lo_sem, hi_sem, r_send, r_recv, m_send, m_recv, h_send, h_recv):
    q = lax.axis_index("wide")
    z = lax.axis_index("narrow")
    slots, params = gs_ref.shape
    size = ls_ref.shape[1]
    groups = params // LANES
    cuts = LANES // CUT
    extra = cuts * nz
    chip, core = q // 2, lax.rem(q, 2)
    steps = 2 * nz

    def peer(step):
        return lax.rem(q + step, nq)

    wide = params // 4
    loads = [pltpu.make_async_copy(weight_hbm, weight_ref, in_sem.at[0]),
             pltpu.make_async_copy(resid_hbm, resid_ref, in_sem.at[1]),
             pltpu.make_async_copy(local_hbm, ls_ref, in_sem.at[2])]
    loads += [pltpu.make_async_copy(global_hbm.at[:, i * wide:(i + 1) * wide], gs_ref.at[:, i * wide:(i + 1) * wide],
                                    in_sem.at[3 + i]) for i in range(4)]
    for copy in loads:
        copy.start()
    barrier = pltpu.get_barrier_semaphore()
    for dz in range(nz):
        for step in range(nq):
            if dz or step:
                pl.semaphore_signal(barrier, inc=1, device_id=(peer(step), lax.rem(z + dz, nz)),
                                    device_id_type=MESH)
    for copy in loads[:3]:
        copy.wait()

    slot = lax.broadcasted_iota(jnp.int32, (1, slots), 1)
    root = jnp.sqrt(jnp.where(slot < count_ref[0], weight_ref[...], 0.0))
    root_col = jnp.broadcast_to(root, (LANES, slots)).T
    rs_col = jnp.broadcast_to(root * resid_ref[...], (LANES, slots)).T
    ls = ls_ref[...] * root_col
    ls_t = ls.T
    eye = (lax.broadcasted_iota(jnp.int32, (size, size), 0)
           == lax.broadcasted_iota(jnp.int32, (size, size), 1)).astype(jnp.float32)
    curv = jnp.dot(ls_t, ls, precision=HIGHEST, preferred_element_type=jnp.float32) + eye
    lr = jnp.sum(ls * rs_col, axis=0, keepdims=True)
    lr_col = jnp.broadcast_to(lr, (LANES, size)).T
    ls_high, ls_low = split(ls_t)
    wide = 2 * LANES

    def couple():
        for g in range(groups):
            cols = slice(g * LANES, (g + 1) * LANES)
            gs = gs_ref[:, cols] * root_col
            high[:, cols], low[:, cols] = split(gs)
            own[g:g + 1, :] = jnp.sum(gs * rs_col, axis=0, keepdims=True)
        for g in range(0, params, wide):
            cols = slice(g, g + wide)
            coupling = (jnp.dot(ls_high, high[:, cols], preferred_element_type=jnp.float32)
                        + (jnp.dot(ls_high, low[:, cols], preferred_element_type=jnp.float32)
                           + jnp.dot(ls_low, high[:, cols], preferred_element_type=jnp.float32)))
            u_ref[:, cols] = coupling
            u_high[:, cols], u_low[:, cols] = split(coupling)

    inverse = invert_panel(curv, 0)
    for copy in loads[3:]:
        copy.wait()
    couple()
    for base in range(PANEL, size, PANEL):
        inverse = invert_panel(inverse, base)

    for g in range(0, params, wide):
        cols = slice(g, g + wide)
        solved = jnp.dot(inverse, u_ref[:, cols], precision=HIGHEST, preferred_element_type=jnp.float32)
        x_high[:, cols], x_low[:, cols] = split(solved)
        for h in range(2):
            r = g // LANES + h
            own[r:r + 1, :] = own[r:r + 1, :] - jnp.sum(
                solved[:, h * LANES:(h + 1) * LANES] * lr_col, axis=0, keepdims=True)
    own[groups:, :] = (lax.broadcasted_iota(jnp.int32, (groups, LANES), 0) == window_ref[0]).astype(jnp.float32)

    def urgency(i, c, a):
        return HOP * abs(i - a) + (MIRROR + abs(a - c) * 0.2 if a != c else 0)

    plans = [[sorted(range(nz), key=lambda a: (-urgency(i, c, a), a)) for c in range(nz)] for i in range(nz)]
    rows_by = [sorted(range(nz), key=lambda a: (sum(plan.index(a) for plan in plans[i]), abs(2 * a - nz + 1) * -1, a)) for i in range(nz)]
    sent_at = [[[max(rows_by[i].index(x) for x in plan[:k + 1]) for k in range(nz)] for plan in plans[i]]
               for i in range(nz)]

    assert all(2 * x + 1 <= 2 * k + AHEAD for rows in sent_at for row in rows for k, x in enumerate(row))

    def here(values):
        total = jnp.int32(0)
        for i in range(nz):
            total = total + jnp.where(z == i, values[i], 0)
        return total

    plan = [[here([plans[i][c][k] for i in range(nz)]) for k in range(nz)] for c in range(nz)]
    group = [[here([sent_at[i][c][k] for i in range(nz)]) for k in range(nz)] for c in range(nz)]
    ways = [3, 1, 2, 0] if nz == 4 else list(range(nz - 1, -1, -1))
    aims = [lax.rem(chip + d, nz) for d in ways]
    plan_to = [[sum(jnp.where(aim == c, plan[c][k], 0) for c in range(nz)) for k in range(nz)] for aim in aims]
    group_to = [[sum(jnp.where(aim == c, group[c][k], 0) for c in range(nz)) for k in range(nz)] for aim in aims]
    row_plan = [here([rows_by[i][k] for i in range(nz)]) for k in range(nz)]
    mine = []
    for k in range(nz):
        total = jnp.int32(0)
        for c in range(nz):
            total = total + jnp.where(chip == c, plan[c][k], 0)
        mine.append(total)

    def pick(values, k):
        total = jnp.int32(0)
        for j in range(nz):
            total = total + jnp.where(k == j, values[j], 0)
        return total

    def goal(k):
        return pick(mine, k)

    def place(a):
        k = jnp.int32(0)
        for j in range(nz):
            k = k + jnp.where(a == mine[j], j, 0)
        return k

    late = cuts * place(chip) + cuts

    def final(i):
        plain = jnp.where(i > late, i - 1, i)
        return jnp.where(i == late, place(chip), jnp.minimum(plain // cuts, nz - 1)) == nz - 1

    def chunk(i):
        plain = jnp.where(i > late, i - 1, i)
        k = jnp.minimum(plain // cuts, nz - 1)
        a = jnp.where(i == late, chip, goal(k))
        return jnp.where(i == late, extra, cuts * a + lax.rem(plain, cuts)), a

    def turn(col, a):
        return jnp.where(col // 2 <= a, lax.rem(col, 2), 1 - lax.rem(col, 2))

    def corner(t, col):
        a = jnp.minimum(t // cuts, nz - 1)
        row = (2 * a + turn(col, a)) * LANES + lax.rem(t, cuts) * CUT
        side = lax.rem(col, 2)
        row = jnp.where(t == extra, (2 * (col // 2) + 1) * LANES + side * CUT, row)
        left = jnp.where(t == extra, col - side, col) * LANES
        return pl.ds(pl.multiple_of(row, CUT), CUT), pl.ds(pl.multiple_of(left, LANES), LANES)

    def plane_copy(t, step):
        rows, cols = corner(t, peer(step))
        return pltpu.make_async_remote_copy(
            src_ref=s_ref.at[rows, cols], dst_ref=recv.at[nq - step, t],
            send_sem=send_sem.at[step, t], recv_sem=recv_sem.at[nq - step, t],
            device_id=(peer(step), z), device_id_type=MESH)

    def small_copy(step):
        return pltpu.make_async_remote_copy(
            src_ref=own, dst_ref=small.at[nq - step],
            send_sem=small_send.at[step], recv_sem=small_recv.at[nq - step],
            device_id=(peer(step), z), device_id_type=MESH)

    def up_copy(t):
        return pltpu.make_async_remote_copy(
            src_ref=part.at[t], dst_ref=from_lo.at[t], send_sem=z_send.at[t], recv_sem=lo_sem.at[t],
            device_id=(q, lax.min(z + 1, nz - 1)), device_id_type=MESH)

    def down_copy(t):
        return pltpu.make_async_remote_copy(
            src_ref=part.at[t], dst_ref=from_hi.at[t], send_sem=z_send.at[t], recv_sem=hi_sem.at[t],
            device_id=(q, lax.max(z - 1, 0)), device_id_type=MESH)

    def rhs_copy(step):
        return pltpu.make_async_remote_copy(
            src_ref=rsum, dst_ref=rrecv.at[nz - step],
            send_sem=r_send.at[step], recv_sem=r_recv.at[nz - step],
            device_id=(q, lax.rem(z + step, nz)), device_id_type=MESH)

    def mirror_copy(cut):
        return pltpu.make_async_remote_copy(
            src_ref=part.at[cuts * z + cut], dst_ref=mirror.at[cut], send_sem=m_send.at[cut], recv_sem=m_recv.at[cut],
            device_id=(2 * z + turn(q, z), chip), device_id_type=MESH)

    def hold_copy():
        return pltpu.make_async_remote_copy(
            src_ref=part.at[cuts * z], dst_ref=hold.at[chip], send_sem=m_send.at[0], recv_sem=h_recv.at[chip],
            device_id=(2 * z + turn(q, z), z), device_id_type=MESH)

    def forward_copy(a):
        return pltpu.make_async_remote_copy(
            src_ref=hold.at[a], dst_ref=mirror.at[0], send_sem=h_send.at[a], recv_sem=m_recv.at[0],
            device_id=(q, a), device_id_type=MESH)

    def arrived(a):
        return pltpu.make_async_remote_copy(
            src_ref=part.at[cuts * z], dst_ref=hold.at[a], send_sem=m_send.at[0], recv_sem=h_recv.at[a],
            device_id=(2 * z + turn(q, z), z), device_id_type=MESH)

    def forward(a):
        @pl.when((chip == z) & (z != a))
        def _():
            arrived(a).wait_recv()
            forward_copy(a).start()

    def swap_copy(cut):
        return pltpu.make_async_remote_copy(
            src_ref=part.at[extra], dst_ref=mirror.at[cut], send_sem=m_send.at[cut], recv_sem=m_recv.at[cut],
            device_id=(q + 1 - 2 * core, z), device_id_type=MESH)

    order = sorted(range(1, nq), key=lambda step: -min(step, nq - step))
    pl.semaphore_wait(barrier, nq * nz - 1)
    for step in order:
        small_copy(step).start()

    def send(i):
        j, h = i // 2, lax.rem(i, 2)
        now = pick(row_plan, j)
        block = pl.ds(pl.multiple_of((2 * now + h) * LANES, LANES), LANES)
        s_ref[block, :] = (three(high[:, block], low[:, block], high[...], low[...])
                           - three(u_high[:, block], u_low[:, block], x_high[...], x_low[...]))
        for d, c in enumerate(aims):
            for k in range(nz):
                a = plan_to[d][k]

                @pl.when(group_to[d][k] == j)
                def _(a=a, c=c):
                    for side in range(2):
                        col = 2 * c + side

                        @pl.when((q != col) & (jnp.where(a == now, turn(col, a), 0) == h))
                        def _(col=col):
                            for cut in range(cuts):
                                plane_copy(cuts * a + cut, lax.rem(col + nq - q, nq)).start()

                        @pl.when((q != col) & (a == c) & (jnp.where(a == now, 1, 0) == h))
                        def _(col=col):
                            plane_copy(extra, lax.rem(col + nq - q, nq)).start()

    def gather(i):
        t, a = chunk(i)
        for step in order:
            plane_copy(t, nq - step).wait_recv()
        rows, cols = corner(t, q)
        recv[0, t] = s_ref[rows, cols]
        for w in range(NWIN):
            total = jnp.zeros((CUT, LANES), jnp.float32)
            for s in range(nq):
                total = total + small[s, groups + w:groups + w + 1, :] * recv[s, t]
            part[t, w] = total

        @pl.when((z == 0) & (a > z))
        def _():
            up_copy(t).start()

        @pl.when((z == nz - 1) & (a < z))
        def _():
            down_copy(t).start()

    def relay(i):
        t, a = chunk(i)

        @pl.when((z > 0) & (a > z))
        def _():
            up_copy(t).wait_recv()
            part[t] = part[t] + from_lo[t]
            up_copy(t).start()

        @pl.when((z < nz - 1) & (a < z))
        def _():
            down_copy(t).wait_recv()
            part[t] = part[t] + from_hi[t]
            down_copy(t).start()

    def finish(i):
        t, a = chunk(i)

        @pl.when(a == z)
        def _():
            @pl.when(z > 0)
            def _():
                up_copy(t).wait_recv()
                part[t] = part[t] + from_lo[t]

            @pl.when(z < nz - 1)
            def _():
                down_copy(t).wait_recv()
                part[t] = part[t] + from_hi[t]

            @pl.when(t == extra)
            def _():
                swap_copy(core).start()

            @pl.when(t != extra)
            def _():
                cut = lax.rem(t, cuts)

                @pl.when((chip != z) & (cut == 0))
                def _():
                    hold_copy().start()

                @pl.when((chip != z) & (cut != 0))
                def _():
                    mirror_copy(cut).start()
                row = turn(q, z) * LANES + cut * CUT
                out_ref[:, pl.ds(pl.multiple_of(row, CUT), CUT), :] = part[t]

    def small_sums():
        small[0] = own[...]
        for step in range(1, nq):
            small_copy(nq - step).wait_recv()
        for w in range(NWIN):
            total = jnp.zeros((groups, LANES), jnp.float32)
            for s in range(nq):
                total = total + small[s, groups + w:groups + w + 1, :] * small[s, :groups, :]
            rsum[w] = total
        for step in range(1, nz):
            rhs_copy(step).start()

    lax.fori_loop(0, AHEAD, lambda i, carry: (send(i), carry)[1], 0)
    small_sums()

    def body(i, carry):
        @pl.when(i + AHEAD < steps)
        def _():
            send(i + AHEAD)

        @pl.when(i <= extra)
        def _():
            gather(i)

        @pl.when(i >= LAG)
        def _():
            relay(i - LAG)

        @pl.when((i >= SETTLE) & jnp.logical_not(final(i - SETTLE)))
        def _():
            finish(i - SETTLE)

        @pl.when((i <= extra) & final(i))
        def _():
            finish(i)

        return carry

    lax.fori_loop(0, extra + 1 + LAG, body, 0)
    for a in range(nz):
        forward(a)

    for step in range(1, nz):
        rhs_copy(nz - step).wait_recv()
    total = rsum[...]
    for step in range(1, nz):
        total = total + rrecv[step]
    rrecv[0] = total
    for w in range(NWIN):
        for h in range(2):
            rhs_ref[w:w + 1, h * LANES:(h + 1) * LANES] = rrecv[0, w, pl.ds(2 * z + h, 1), :]

    @pl.when(chip != z)
    def _():
        for cut in range(cuts):
            mirror_copy(cut).wait_recv()
        row = (1 - turn(q, z)) * LANES
        for w in range(NWIN):
            block = jnp.concatenate([mirror[cut, w] for cut in range(cuts)], axis=0)
            out_ref[w, pl.ds(pl.multiple_of(row, LANES), LANES), :] = block.T

    for side in range(2):
        @pl.when((chip == z) & (core == side))
        def _(side=side):
            swap_copy(1 - side).wait_recv()
            for w in range(NWIN):
                pieces = [part[extra, w] if cut == side else mirror[cut, w] for cut in range(cuts)]
                block = jnp.concatenate(pieces, axis=0)
                out_ref[w, (1 - side) * LANES:(2 - side) * LANES, :] = block.T if side else block

    for step in range(1, nq):
        small_copy(step).wait_send()
    for step in range(1, nz):
        rhs_copy(step).wait_send()

    @pl.when(chip != z)
    def _():
        for cut in range(cuts):
            mirror_copy(cut).wait_send()

    @pl.when(chip == z)
    def _():
        swap_copy(core).wait_send()
        for a in range(nz):
            @pl.when(z != a)
            def _(a=a):
                forward_copy(a).wait_send()

    def drain(t, carry):
        for step in range(1, nq):
            plane_copy(t, step).wait_send()
        a = jnp.where(t == extra, chip, t // cuts)

        @pl.when(a != z)
        def _():
            up_copy(t).wait_send()
        return carry

    lax.fori_loop(0, extra + 1, drain, 0)


def assemble(nq, nz, count, window, local_b, global_b, resid, weight):
    slots, params = global_b.shape
    size = local_b.shape[1]
    groups = params // LANES
    cuts = LANES // CUT
    chunks = cuts * nz + 1
    smem = pl.BlockSpec(memory_space=pltpu.SMEM)
    hbm = pl.BlockSpec(memory_space=pltpu.HBM)
    vmem = pl.BlockSpec(memory_space=pltpu.VMEM)
    f32, bf16 = jnp.float32, jnp.bfloat16
    block = pltpu.VMEM((chunks, NWIN, CUT, LANES), f32)
    dma = pltpu.SemaphoreType.DMA
    return pl.pallas_call(
        functools.partial(assemble_kernel, nq, nz),
        out_shape=(jax.ShapeDtypeStruct((NWIN, params // nz, LANES), f32),
                   jax.ShapeDtypeStruct((NWIN, params // nz), f32)),
        in_specs=[smem] * 2 + [hbm] * 4,
        out_specs=(vmem, vmem),
        scratch_shapes=[
            pltpu.VMEM((slots, size), f32), pltpu.VMEM((slots, params), f32),
            pltpu.VMEM((1, slots), f32), pltpu.VMEM((1, slots), f32),
            pltpu.VMEM((slots, params), bf16), pltpu.VMEM((slots, params), bf16),
            pltpu.VMEM((size, params), f32),
            pltpu.VMEM((size, params), bf16), pltpu.VMEM((size, params), bf16),
            pltpu.VMEM((size, params), bf16), pltpu.VMEM((size, params), bf16),
            pltpu.VMEM((params, params), f32),
            pltpu.VMEM((2 * groups, LANES), f32),
            pltpu.VMEM((nq, chunks, CUT, LANES), f32),
            pltpu.VMEM((nq, 2 * groups, LANES), f32),
            block, block, block,
            pltpu.VMEM((cuts, NWIN, CUT, LANES), f32), pltpu.VMEM((nz, NWIN, CUT, LANES), f32),
            pltpu.VMEM((NWIN, groups, LANES), f32),
            pltpu.VMEM((nz, NWIN, groups, LANES), f32),
            dma((7,)), dma((nq, chunks)), dma((nq, chunks)), dma((nq,)), dma((nq,)),
            dma((chunks,)), dma((chunks,)), dma((chunks,)), dma((nz,)), dma((nz,)),
            dma((cuts,)), dma((cuts,)), dma((nz,)), dma((nz,)),
        ],
        compiler_params=pltpu.CompilerParams(
            collective_id=0, has_side_effects=True, vmem_limit_bytes=48 * 1024 * 1024),
        name="assemble",
    )(count, window, *(pltpu.with_memory_space_constraint(x, pltpu.HBM) for x in (local_b, global_b, resid, weight)))


def reduced_bundle(local_b, global_b, resid_b, weight_b, count):
    measure_slot, local_param = local_b.shape
    slots = jnp.arange(measure_slot, dtype=jnp.int32)
    live = jnp.where(slots < count, weight_b, jnp.float32(0.0))
    root = jnp.sqrt(live)[:, None]
    ls = local_b * root
    gs = global_b * root
    rs = resid_b[:, None] * root
    curv = tdot(ls, ls) + jnp.eye(local_param, dtype=jnp.float32)
    coupling = tdot(ls, gs)
    lr = tdot(ls, rs)
    gr = tdot(gs, rs)[:, 0]
    factor = jnp.linalg.cholesky(curv)
    solved_all = jax.scipy.linalg.cho_solve((factor, True), jnp.concatenate([coupling, lr], axis=1))
    solved, solved_rhs = solved_all[:, :-1], solved_all[:, -1:]
    schur = tdot(gs, gs, HIGH) - tdot(coupling, solved, HIGH)
    reduced = gr - tdot(coupling, solved_rhs)[:, 0]
    return schur, reduced


def on_device(local_slopes, global_slopes, residuals, weights, track_slot_count, windows):
    nq, nz = lax.axis_size("wide"), lax.axis_size("narrow")
    slots, params = global_slopes.shape[1:]
    owned = params // nz
    z = lax.axis_index("narrow")
    if params // nq == LANES and local_slopes.shape[2] == LANES and nq == 2 * nz and nz > 1:
        return assemble(nq, nz, track_slot_count, windows, local_slopes[0], global_slopes[0], residuals, weights)
    schur, reduced = reduced_bundle(
        local_slopes[0], global_slopes[0], residuals[0], weights[0], track_slot_count[0])
    picks = (windows[0] == jnp.arange(NWIN, dtype=jnp.int32)).astype(jnp.float32)
    rhs_whole = lax.psum(picks[:, None] * reduced[None], ("wide", "narrow"))
    normal_rhs = lax.dynamic_slice_in_dim(rhs_whole, z * owned, owned, 1)
    received = lax.all_to_all(schur[None], "wide", split_axis=2, concat_axis=0, tiled=True)
    all_picks = lax.all_gather(picks, "wide", axis=0)
    partial_value = jnp.einsum("bw,bij->wij", all_picks, received, precision=HIGHEST,
                               preferred_element_type=jnp.float32)
    return lax.psum_scatter(partial_value, "narrow", scatter_dimension=1, tiled=True), normal_rhs


def solution(mesh):
    in_specs = (
        P(("wide", "narrow"), None, None),
        P(("wide", "narrow"), None, None),
        P(("wide", "narrow"), None),
        P(("wide", "narrow"), None),
        P(("wide", "narrow")),
        P(("wide", "narrow")),
    )
    out_specs = (P(None, "narrow", "wide"), P(None, "narrow"))
    return jax.shard_map(
        on_device, mesh=mesh, in_specs=in_specs, out_specs=out_specs, check_vma=False
    )
```

```python
import functools
import jax
import jax.numpy as jnp
from jax import lax
from jax.experimental import pallas as pl
from jax.experimental.pallas import tpu as pltpu
from jax.sharding import PartitionSpec as P

WINDOW_PARAMS = 1024
NWIN = 4
LANES = 128
SUB = 8
PANEL = 32
CUT = 64
AHEAD = 4
LAG = 1
PARTS = 2
SETTLE = 3
HOP = 3
MIRROR = -0.8
MESH = pl.DeviceIdType.MESH
HIGHEST = lax.Precision.HIGHEST
HIGH = lax.Precision.HIGH


def tdot(left, right, precision=HIGHEST):
    return lax.dot_general(
        left,
        right,
        (((0,), (0,)), ((), ())),
        precision=precision,
        preferred_element_type=jnp.float32,
    )


def eliminate(rows, base):
    size = rows[0].shape[1]
    sub = lax.broadcasted_iota(jnp.int32, (SUB, size), 0)
    lane = lax.broadcasted_iota(jnp.int32, (SUB, size), 1)

    def row(x, k):
        return jnp.broadcast_to(x[k:k + 1, :], (SUB, size))

    for r in range(len(rows)):
        first = base + SUB * r
        cols = [[jnp.broadcast_to(x[:, first + j:first + j + 1], (SUB, size)) for j in range(SUB)] for x in rows]
        pivot, panel = list(cols[r]), rows[r]
        for k in range(0, SUB, 2):
            u, v = pivot[k], pivot[k + 1]
            a, c, b, d = row(u, k), row(u, k + 1), row(v, k), row(v, k + 1)
            inv = 1.0 / (a * d - b * c)

            def step(x, here=None, after=None):
                r0, r1 = row(x, k), row(x, k + 1)
                if here is not None:
                    r0 = jnp.where(here, 1.0, jnp.where(after, 0.0, r0))
                    r1 = jnp.where(after, 1.0, jnp.where(here, 0.0, r1))
                    x = jnp.where(here | after, 0.0, x)
                p0 = (d * r0 - b * r1) * inv
                p1 = (a * r1 - c * r0) * inv
                x = x - u * p0 - v * p1
                return jnp.where(sub == k, p0, jnp.where(sub == k + 1, p1, x))

            for j in range(k + 2, SUB):
                pivot[j] = step(pivot[j])
            panel = step(panel, lane == first + k, lane == first + k + 1)
        inside = (lane >= first) & (lane < first + SUB)
        heads = [row(panel, j) for j in range(SUB)]
        for i in range(len(rows)):
            if i != r:
                t = [cols[i][j] * heads[j] for j in range(SUB)]
                rows[i] = jnp.where(inside, 0.0, rows[i]) - (
                    ((t[0] + t[1]) + (t[2] + t[3])) + ((t[4] + t[5]) + (t[6] + t[7])))
        rows[r] = panel
    return jnp.concatenate(rows, axis=0)


def invert_panel(c, base):
    size = c.shape[0]
    lane = lax.broadcasted_iota(jnp.int32, (1, size), 1)
    end = base + PANEL
    panel = eliminate([c[i:i + SUB, :] for i in range(base, end, SUB)], base)

    def framed(above, below):
        return jnp.concatenate([x for x in (above, panel, below) if x.shape[0]], axis=0)

    heads = framed(jnp.zeros((base, size), jnp.float32), jnp.zeros((size - end, size), jnp.float32))
    taken = jnp.dot(c, heads, precision=HIGHEST, preferred_element_type=jnp.float32)
    rest = jnp.where((lane >= base) & (lane < end), 0.0, c) - taken
    return framed(rest[:base, :], rest[end:, :])


def split(x):
    high = x.astype(jnp.bfloat16)
    return high, (x - high.astype(jnp.float32)).astype(jnp.bfloat16)


def product(left, right):
    return lax.dot_general(left, right, (((0,), (0,)), ((), ())), preferred_element_type=jnp.float32)


def three(left_high, left_low, right_high, right_low):
    return product(left_high, right_high) + (product(left_high, right_low) + product(left_low, right_high))


def assemble_kernel(nq, nz, count_ref, window_ref, local_hbm, global_hbm, resid_hbm, weight_hbm,
                    out_ref, rhs_ref,
                    ls_ref, gs_ref, resid_ref, weight_ref, high, low, u_ref, u_high, u_low, x_high, x_low,
                    s_ref, own, recv, small, part, from_lo, from_hi, mirror, hold, rsum, rrecv,
                    in_sem, send_sem, recv_sem, small_send, small_recv,
                    z_send, lo_sem, hi_sem, r_send, r_recv, m_send, m_recv, h_send, h_recv, m_half, m_part):
    q = lax.axis_index("wide")
    z = lax.axis_index("narrow")
    slots, params = gs_ref.shape
    size = ls_ref.shape[1]
    groups = params // LANES
    cuts = LANES // CUT
    extra = cuts * nz
    chip, core = q // 2, lax.rem(q, 2)
    steps = 2 * nz

    def peer(step):
        return lax.rem(q + step, nq)

    wide = params // 4
    loads = [pltpu.make_async_copy(weight_hbm, weight_ref, in_sem.at[0]),
             pltpu.make_async_copy(resid_hbm, resid_ref, in_sem.at[1]),
             pltpu.make_async_copy(local_hbm, ls_ref, in_sem.at[2])]
    loads += [pltpu.make_async_copy(global_hbm.at[:, i * wide:(i + 1) * wide], gs_ref.at[:, i * wide:(i + 1) * wide],
                                    in_sem.at[3 + i]) for i in range(4)]
    for copy in loads:
        copy.start()
    barrier = pltpu.get_barrier_semaphore()
    for dz in range(nz):
        for step in range(nq):
            if dz or step:
                pl.semaphore_signal(barrier, inc=1, device_id=(peer(step), lax.rem(z + dz, nz)),
                                    device_id_type=MESH)
    for copy in loads[:3]:
        copy.wait()

    slot = lax.broadcasted_iota(jnp.int32, (1, slots), 1)
    root = jnp.sqrt(jnp.where(slot < count_ref[0], weight_ref[...], 0.0))
    root_col = jnp.broadcast_to(root, (LANES, slots)).T
    rs_col = jnp.broadcast_to(root * resid_ref[...], (LANES, slots)).T
    ls = ls_ref[...] * root_col
    ls_t = ls.T
    eye = (lax.broadcasted_iota(jnp.int32, (size, size), 0)
           == lax.broadcasted_iota(jnp.int32, (size, size), 1)).astype(jnp.float32)
    curv = jnp.dot(ls_t, ls, precision=HIGHEST, preferred_element_type=jnp.float32) + eye
    lr = jnp.sum(ls * rs_col, axis=0, keepdims=True)
    lr_col = jnp.broadcast_to(lr, (LANES, size)).T
    ls_high, ls_low = split(ls_t)
    wide = 2 * LANES

    def couple():
        for g in range(groups):
            cols = slice(g * LANES, (g + 1) * LANES)
            gs = gs_ref[:, cols] * root_col
            high[:, cols], low[:, cols] = split(gs)
            own[g:g + 1, :] = jnp.sum(gs * rs_col, axis=0, keepdims=True)
        for g in range(0, params, wide):
            cols = slice(g, g + wide)
            coupling = (jnp.dot(ls_high, high[:, cols], preferred_element_type=jnp.float32)
                        + (jnp.dot(ls_high, low[:, cols], preferred_element_type=jnp.float32)
                           + jnp.dot(ls_low, high[:, cols], preferred_element_type=jnp.float32)))
            u_ref[:, cols] = coupling
            u_high[:, cols], u_low[:, cols] = split(coupling)

    inverse = invert_panel(invert_panel(curv, 0), PANEL)
    for copy in loads[3:]:
        copy.wait()
    couple()
    for base in range(2 * PANEL, size, PANEL):
        inverse = invert_panel(inverse, base)

    for g in range(0, params, wide):
        cols = slice(g, g + wide)
        solved = jnp.dot(inverse, u_ref[:, cols], precision=HIGHEST, preferred_element_type=jnp.float32)
        x_high[:, cols], x_low[:, cols] = split(solved)
        for h in range(2):
            r = g // LANES + h
            own[r:r + 1, :] = own[r:r + 1, :] - jnp.sum(
                solved[:, h * LANES:(h + 1) * LANES] * lr_col, axis=0, keepdims=True)
    own[groups:, :] = (lax.broadcasted_iota(jnp.int32, (groups, LANES), 0) == window_ref[0]).astype(jnp.float32)

    def urgency(i, c, a):
        return HOP * abs(i - a) + (MIRROR + abs(a - c) * 0.2 if a != c else 0)

    plans = [[sorted(range(nz), key=lambda a: (-urgency(i, c, a), a)) for c in range(nz)] for i in range(nz)]
    rows_by = [sorted(range(nz), key=lambda a: (sum(plan.index(a) for plan in plans[i]), abs(2 * a - nz + 1) * -1, a)) for i in range(nz)]
    sent_at = [[[max(rows_by[i].index(x) for x in plan[:k + 1]) for k in range(nz)] for plan in plans[i]]
               for i in range(nz)]

    assert all(2 * x + 1 <= 2 * k + AHEAD for rows in sent_at for row in rows for k, x in enumerate(row))

    def here(values):
        total = jnp.int32(0)
        for i in range(nz):
            total = total + jnp.where(z == i, values[i], 0)
        return total

    plan = [[here([plans[i][c][k] for i in range(nz)]) for k in range(nz)] for c in range(nz)]
    group = [[here([sent_at[i][c][k] for i in range(nz)]) for k in range(nz)] for c in range(nz)]
    ways = [3, 1, 2, 0] if nz == 4 else list(range(nz - 1, -1, -1))
    aims = [lax.rem(chip + d, nz) for d in ways]
    plan_to = [[sum(jnp.where(aim == c, plan[c][k], 0) for c in range(nz)) for k in range(nz)] for aim in aims]
    group_to = [[sum(jnp.where(aim == c, group[c][k], 0) for c in range(nz)) for k in range(nz)] for aim in aims]
    row_plan = [here([rows_by[i][k] for i in range(nz)]) for k in range(nz)]
    mine = []
    for k in range(nz):
        total = jnp.int32(0)
        for c in range(nz):
            total = total + jnp.where(chip == c, plan[c][k], 0)
        mine.append(total)

    def pick(values, k):
        total = jnp.int32(0)
        for j in range(nz):
            total = total + jnp.where(k == j, values[j], 0)
        return total

    def goal(k):
        return pick(mine, k)

    def place(a):
        k = jnp.int32(0)
        for j in range(nz):
            k = k + jnp.where(a == mine[j], j, 0)
        return k

    late = cuts * place(chip) + cuts

    def final(i):
        plain = jnp.where(i > late, i - 1, i)
        return jnp.where(i == late, place(chip), jnp.minimum(plain // cuts, nz - 1)) == nz - 1

    def chunk(i):
        plain = jnp.where(i > late, i - 1, i)
        k = jnp.minimum(plain // cuts, nz - 1)
        a = jnp.where(i == late, chip, goal(k))
        return jnp.where(i == late, extra, cuts * a + lax.rem(plain, cuts)), a

    def turn(col, a):
        return jnp.where(col // 2 <= a, lax.rem(col, 2), 1 - lax.rem(col, 2))

    def corner(t, col):
        a = jnp.minimum(t // cuts, nz - 1)
        row = (2 * a + turn(col, a)) * LANES + lax.rem(t, cuts) * CUT
        side = lax.rem(col, 2)
        row = jnp.where(t == extra, (2 * (col // 2) + 1) * LANES + side * CUT, row)
        left = jnp.where(t == extra, col - side, col) * LANES
        return pl.ds(pl.multiple_of(row, CUT), CUT), pl.ds(pl.multiple_of(left, LANES), LANES)

    def plane_copy(t, step):
        rows, cols = corner(t, peer(step))
        return pltpu.make_async_remote_copy(
            src_ref=s_ref.at[rows, cols], dst_ref=recv.at[nq - step, t],
            send_sem=send_sem.at[step, t], recv_sem=recv_sem.at[nq - step, t],
            device_id=(peer(step), z), device_id_type=MESH)

    def small_copy(step):
        return pltpu.make_async_remote_copy(
            src_ref=own, dst_ref=small.at[nq - step],
            send_sem=small_send.at[step], recv_sem=small_recv.at[nq - step],
            device_id=(peer(step), z), device_id_type=MESH)

    def up_copy(t):
        return pltpu.make_async_remote_copy(
            src_ref=part.at[t], dst_ref=from_lo.at[t], send_sem=z_send.at[t], recv_sem=lo_sem.at[t],
            device_id=(q, lax.min(z + 1, nz - 1)), device_id_type=MESH)

    def down_copy(t):
        return pltpu.make_async_remote_copy(
            src_ref=part.at[t], dst_ref=from_hi.at[t], send_sem=z_send.at[t], recv_sem=hi_sem.at[t],
            device_id=(q, lax.max(z - 1, 0)), device_id_type=MESH)

    def rhs_copy(step):
        return pltpu.make_async_remote_copy(
            src_ref=rsum, dst_ref=rrecv.at[nz - step],
            send_sem=r_send.at[step], recv_sem=r_recv.at[nz - step],
            device_id=(q, lax.rem(z + step, nz)), device_id_type=MESH)

    def mirror_copy(cut):
        return pltpu.make_async_remote_copy(
            src_ref=part.at[cuts * z + cut], dst_ref=mirror.at[cut], send_sem=m_send.at[cut], recv_sem=m_recv.at[cut],
            device_id=(2 * z + turn(q, z), chip), device_id_type=MESH)

    def share(p):
        return pl.ds(p * (NWIN // PARTS), NWIN // PARTS)

    def arrived(a, p):
        return pltpu.make_async_remote_copy(
            src_ref=part.at[cuts * z, share(p)], dst_ref=hold.at[a, share(p)],
            send_sem=m_half.at[p], recv_sem=h_recv.at[a, p],
            device_id=(2 * z + turn(q, z), z), device_id_type=MESH)

    def hold_copy(p):
        return arrived(chip, p)

    def forward_copy(a, p):
        return pltpu.make_async_remote_copy(
            src_ref=hold.at[a, share(p)], dst_ref=mirror.at[0, share(p)],
            send_sem=h_send.at[a, p], recv_sem=m_part.at[p],
            device_id=(q, a), device_id_type=MESH)

    def forward(a):
        @pl.when((chip == z) & (z != a))
        def _():
            for p in range(PARTS):
                arrived(a, p).wait_recv()
                forward_copy(a, p).start()

    def swap_copy(cut):
        return pltpu.make_async_remote_copy(
            src_ref=part.at[extra], dst_ref=mirror.at[cut], send_sem=m_send.at[cut], recv_sem=m_recv.at[cut],
            device_id=(q + 1 - 2 * core, z), device_id_type=MESH)

    order = sorted(range(1, nq), key=lambda step: -min(step, nq - step))
    pl.semaphore_wait(barrier, nq * nz - 1)
    for step in order:
        small_copy(step).start()

    def send(i):
        j, h = i // 2, lax.rem(i, 2)
        now = pick(row_plan, j)
        block = pl.ds(pl.multiple_of((2 * now + h) * LANES, LANES), LANES)
        s_ref[block, :] = (three(high[:, block], low[:, block], high[...], low[...])
                           - three(u_high[:, block], u_low[:, block], x_high[...], x_low[...]))
        for d, c in enumerate(aims):
            for k in range(nz):
                a = plan_to[d][k]

                @pl.when(group_to[d][k] == j)
                def _(a=a, c=c):
                    for side in range(2):
                        col = 2 * c + side

                        @pl.when((q != col) & (jnp.where(a == now, turn(col, a), 0) == h))
                        def _(col=col):
                            for cut in range(cuts):
                                plane_copy(cuts * a + cut, lax.rem(col + nq - q, nq)).start()

                        @pl.when((q != col) & (a == c) & (jnp.where(a == now, 1, 0) == h))
                        def _(col=col):
                            plane_copy(extra, lax.rem(col + nq - q, nq)).start()

    def gather(i):
        t, a = chunk(i)
        for step in order:
            plane_copy(t, nq - step).wait_recv()
        rows, cols = corner(t, q)
        recv[0, t] = s_ref[rows, cols]
        for w in range(NWIN):
            total = jnp.zeros((CUT, LANES), jnp.float32)
            for s in range(nq):
                total = total + small[s, groups + w:groups + w + 1, :] * recv[s, t]
            part[t, w] = total

        @pl.when((z == 0) & (a > z))
        def _():
            up_copy(t).start()

        @pl.when((z == nz - 1) & (a < z))
        def _():
            down_copy(t).start()

    def relay(i):
        t, a = chunk(i)

        @pl.when((z > 0) & (a > z))
        def _():
            up_copy(t).wait_recv()
            part[t] = part[t] + from_lo[t]
            up_copy(t).start()

        @pl.when((z < nz - 1) & (a < z))
        def _():
            down_copy(t).wait_recv()
            part[t] = part[t] + from_hi[t]
            down_copy(t).start()

    def finish(i):
        t, a = chunk(i)

        @pl.when(a == z)
        def _():
            @pl.when(z > 0)
            def _():
                up_copy(t).wait_recv()
                part[t] = part[t] + from_lo[t]

            @pl.when(z < nz - 1)
            def _():
                down_copy(t).wait_recv()
                part[t] = part[t] + from_hi[t]

            @pl.when(t == extra)
            def _():
                swap_copy(core).start()

            @pl.when(t != extra)
            def _():
                cut = lax.rem(t, cuts)

                @pl.when((chip != z) & (cut == 0))
                def _():
                    for p in range(PARTS):
                        hold_copy(p).start()

                @pl.when((chip != z) & (cut != 0))
                def _():
                    mirror_copy(cut).start()
                row = turn(q, z) * LANES + cut * CUT
                out_ref[:, pl.ds(pl.multiple_of(row, CUT), CUT), :] = part[t]

    def small_sums():
        small[0] = own[...]
        for step in range(1, nq):
            small_copy(nq - step).wait_recv()
        for w in range(NWIN):
            total = jnp.zeros((groups, LANES), jnp.float32)
            for s in range(nq):
                total = total + small[s, groups + w:groups + w + 1, :] * small[s, :groups, :]
            rsum[w] = total
        for step in range(1, nz):
            rhs_copy(step).start()

    lax.fori_loop(0, AHEAD, lambda i, carry: (send(i), carry)[1], 0)
    small_sums()

    def body(i, carry):
        @pl.when(i + AHEAD < steps)
        def _():
            send(i + AHEAD)

        @pl.when(i <= extra)
        def _():
            gather(i)

        @pl.when(i >= LAG)
        def _():
            relay(i - LAG)

        @pl.when((i >= SETTLE) & jnp.logical_not(final(i - SETTLE)))
        def _():
            finish(i - SETTLE)

        @pl.when((i <= extra) & final(i))
        def _():
            finish(i)

        return carry

    lax.fori_loop(0, extra + 1 + LAG, body, 0)
    for a in range(nz):
        forward(a)

    for step in range(1, nz):
        rhs_copy(nz - step).wait_recv()
    total = rsum[...]
    for step in range(1, nz):
        total = total + rrecv[step]
    rrecv[0] = total
    for w in range(NWIN):
        for h in range(2):
            rhs_ref[w:w + 1, h * LANES:(h + 1) * LANES] = rrecv[0, w, pl.ds(2 * z + h, 1), :]

    @pl.when(chip != z)
    def _():
        for cut in range(1, cuts):
            mirror_copy(cut).wait_recv()
        for p in range(PARTS):
            forward_copy(0, p).wait_recv()
        row = (1 - turn(q, z)) * LANES
        for w in range(NWIN):
            block = jnp.concatenate([mirror[cut, w] for cut in range(cuts)], axis=0)
            out_ref[w, pl.ds(pl.multiple_of(row, LANES), LANES), :] = block.T

    for side in range(2):
        @pl.when((chip == z) & (core == side))
        def _(side=side):
            swap_copy(1 - side).wait_recv()
            for w in range(NWIN):
                pieces = [part[extra, w] if cut == side else mirror[cut, w] for cut in range(cuts)]
                block = jnp.concatenate(pieces, axis=0)
                out_ref[w, (1 - side) * LANES:(2 - side) * LANES, :] = block.T if side else block

    for step in range(1, nq):
        small_copy(step).wait_send()
    for step in range(1, nz):
        rhs_copy(step).wait_send()

    @pl.when(chip != z)
    def _():
        for cut in range(1, cuts):
            mirror_copy(cut).wait_send()
        for p in range(PARTS):
            hold_copy(p).wait_send()

    @pl.when(chip == z)
    def _():
        swap_copy(core).wait_send()
        for a in range(nz):
            @pl.when(z != a)
            def _(a=a):
                for p in range(PARTS):
                    forward_copy(a, p).wait_send()

    def drain(t, carry):
        for step in range(1, nq):
            plane_copy(t, step).wait_send()
        a = jnp.where(t == extra, chip, t // cuts)

        @pl.when(a != z)
        def _():
            up_copy(t).wait_send()
        return carry

    lax.fori_loop(0, extra + 1, drain, 0)


def assemble(nq, nz, count, window, local_b, global_b, resid, weight):
    slots, params = global_b.shape
    size = local_b.shape[1]
    groups = params // LANES
    cuts = LANES // CUT
    chunks = cuts * nz + 1
    smem = pl.BlockSpec(memory_space=pltpu.SMEM)
    hbm = pl.BlockSpec(memory_space=pltpu.HBM)
    vmem = pl.BlockSpec(memory_space=pltpu.VMEM)
    f32, bf16 = jnp.float32, jnp.bfloat16
    block = pltpu.VMEM((chunks, NWIN, CUT, LANES), f32)
    dma = pltpu.SemaphoreType.DMA
    return pl.pallas_call(
        functools.partial(assemble_kernel, nq, nz),
        out_shape=(jax.ShapeDtypeStruct((NWIN, params // nz, LANES), f32),
                   jax.ShapeDtypeStruct((NWIN, params // nz), f32)),
        in_specs=[smem] * 2 + [hbm] * 4,
        out_specs=(vmem, vmem),
        scratch_shapes=[
            pltpu.VMEM((slots, size), f32), pltpu.VMEM((slots, params), f32),
            pltpu.VMEM((1, slots), f32), pltpu.VMEM((1, slots), f32),
            pltpu.VMEM((slots, params), bf16), pltpu.VMEM((slots, params), bf16),
            pltpu.VMEM((size, params), f32),
            pltpu.VMEM((size, params), bf16), pltpu.VMEM((size, params), bf16),
            pltpu.VMEM((size, params), bf16), pltpu.VMEM((size, params), bf16),
            pltpu.VMEM((params, params), f32),
            pltpu.VMEM((2 * groups, LANES), f32),
            pltpu.VMEM((nq, chunks, CUT, LANES), f32),
            pltpu.VMEM((nq, 2 * groups, LANES), f32),
            block, block, block,
            pltpu.VMEM((cuts, NWIN, CUT, LANES), f32), pltpu.VMEM((nz, NWIN, CUT, LANES), f32),
            pltpu.VMEM((NWIN, groups, LANES), f32),
            pltpu.VMEM((nz, NWIN, groups, LANES), f32),
            dma((7,)), dma((nq, chunks)), dma((nq, chunks)), dma((nq,)), dma((nq,)),
            dma((chunks,)), dma((chunks,)), dma((chunks,)), dma((nz,)), dma((nz,)),
            dma((cuts,)), dma((cuts,)), dma((nz, PARTS)), dma((nz, PARTS)), dma((PARTS,)), dma((PARTS,)),
        ],
        compiler_params=pltpu.CompilerParams(
            collective_id=0, has_side_effects=True, vmem_limit_bytes=48 * 1024 * 1024),
        name="assemble",
    )(count, window, *(pltpu.with_memory_space_constraint(x, pltpu.HBM) for x in (local_b, global_b, resid, weight)))


def reduced_bundle(local_b, global_b, resid_b, weight_b, count):
    measure_slot, local_param = local_b.shape
    slots = jnp.arange(measure_slot, dtype=jnp.int32)
    live = jnp.where(slots < count, weight_b, jnp.float32(0.0))
    root = jnp.sqrt(live)[:, None]
    ls = local_b * root
    gs = global_b * root
    rs = resid_b[:, None] * root
    curv = tdot(ls, ls) + jnp.eye(local_param, dtype=jnp.float32)
    coupling = tdot(ls, gs)
    lr = tdot(ls, rs)
    gr = tdot(gs, rs)[:, 0]
    factor = jnp.linalg.cholesky(curv)
    solved_all = jax.scipy.linalg.cho_solve((factor, True), jnp.concatenate([coupling, lr], axis=1))
    solved, solved_rhs = solved_all[:, :-1], solved_all[:, -1:]
    schur = tdot(gs, gs, HIGH) - tdot(coupling, solved, HIGH)
    reduced = gr - tdot(coupling, solved_rhs)[:, 0]
    return schur, reduced


def on_device(local_slopes, global_slopes, residuals, weights, track_slot_count, windows):
    nq, nz = lax.axis_size("wide"), lax.axis_size("narrow")
    slots, params = global_slopes.shape[1:]
    owned = params // nz
    z = lax.axis_index("narrow")
    if params // nq == LANES and local_slopes.shape[2] == LANES and nq == 2 * nz and nz > 1:
        return assemble(nq, nz, track_slot_count, windows, local_slopes[0], global_slopes[0], residuals, weights)
    schur, reduced = reduced_bundle(
        local_slopes[0], global_slopes[0], residuals[0], weights[0], track_slot_count[0])
    picks = (windows[0] == jnp.arange(NWIN, dtype=jnp.int32)).astype(jnp.float32)
    rhs_whole = lax.psum(picks[:, None] * reduced[None], ("wide", "narrow"))
    normal_rhs = lax.dynamic_slice_in_dim(rhs_whole, z * owned, owned, 1)
    received = lax.all_to_all(schur[None], "wide", split_axis=2, concat_axis=0, tiled=True)
    all_picks = lax.all_gather(picks, "wide", axis=0)
    partial_value = jnp.einsum("bw,bij->wij", all_picks, received, precision=HIGHEST,
                               preferred_element_type=jnp.float32)
    return lax.psum_scatter(partial_value, "narrow", scatter_dimension=1, tiled=True), normal_rhs


def solution(mesh):
    in_specs = (
        P(("wide", "narrow"), None, None),
        P(("wide", "narrow"), None, None),
        P(("wide", "narrow"), None),
        P(("wide", "narrow"), None),
        P(("wide", "narrow")),
        P(("wide", "narrow")),
    )
    out_specs = (P(None, "narrow", "wide"), P(None, "narrow"))
    return jax.shard_map(
        on_device, mesh=mesh, in_specs=in_specs, out_specs=out_specs, check_vma=False
    )
```
